32 devices in a mesh: pair: 16 (over z, y, x), sector: 2 (over core).
Axes of the slice: x: 2, y: 2, z: 4, core: 2. Of those that a mesh axis runs over, the one named last changes fastest.
Arguments:
- wavefunction: float32 [2, 512, 512], P('sector', 'pair'), may hold values from -6 to 6
- preconditioner: float32 [2, 512, 512], P('sector', 'pair'), may hold values from 0.5 to 4
- left_ops: float32 [48, 2, 512, 512], P('pair', 'sector'), may hold values from -0.25 to 0.25
- right_ops: float32 [48, 2, 512, 512], P('pair', 'sector'), may hold values from -0.02734375 to 0.02734375
- charges: int32 [48], P('pair'), may hold values from 0 to 2
- coupling: int32 [2, 3], P('sector'), may hold values 0 or 1
Outputs:
- new_state: float32 [2, 512, 512], P('sector', 'pair')
- new_image: float32 [2, 512, 512], P('sector', 'pair')
- energies: float32 [2], replicated
The draws below stay inside these ranges and needn't reach their ends.
All inputs are finite; a program needn't handle non-finite values. No bound on the sum of `coupling` on one device may be relied on, other than what follows from the above.
Results may differ from the reference program's by a relative error of at most 0.0003.
Values sent between devices are 32-bit elements; how exact they have to be, the bound alone decides.
No kernel may reach another device: no remote copies, remote signals or barrier semaphores. Data moves between devices by JAX's collectives and lax.ppermute only.
A program may use at most 64 MiB of HBM per device.

```python
import math
import jax
import jax.numpy as jnp
from jax import lax

M = 512
PAIRS = 48
SECTORS = 2


def place_ends(entries, rng, smallest, high):
    shape = entries.shape
    place = [jax.random.randint(jax.random.fold_in(rng, axis), (), 0, shape[axis]) for axis in range(len(shape))]
    entries = entries.at[tuple(place)].set(smallest)
    longest = shape.index(max(shape))
    place[longest] = (place[longest] + 1) % shape[longest]
    return entries.at[tuple(place)].set(high)


def shard_levels(rng, extent, shards, low, top_value):
    level = 1.0
    for axis_at, parts in shards:
        steps = jax.random.uniform(jax.random.fold_in(jax.random.fold_in(rng, 6), axis_at), (parts,), jnp.float32, low / len(shards), top_value / len(shards))
        level = level * jnp.repeat(jnp.exp(steps), extent[axis_at] // parts).reshape((-1,) + (1,) * (len(extent) - 1 - axis_at))
    return level


def noise(key, shape, scale, limit, split=(), kind=jnp.bfloat16):
    gain = shard_levels(key, shape, split, -0.22, 0.18) if split else 1.0
    values = jax.random.normal(key, shape, jnp.float32) * scale * gain
    return jnp.minimum(jnp.maximum(values, -limit), limit).astype(kind)


def setup_inputs(seed: int = 0) -> dict:
    keys = jax.random.split(jax.random.key(seed), 7)
    wavefunction = noise(keys[0], (SECTORS, M, M), 1.0, 6.0, ((0, 2), (1, 16)), jnp.float32)
    preconditioner = jnp.clip(jnp.exp(math.log(4.0) - 2.0794415 * jax.random.uniform(keys[1], (SECTORS, M, M), jnp.float32) ** shard_levels(keys[1], (SECTORS, M, M), ((0, 2), (1, 16)), -0.2, 0.2)), 0.5, 4.0)
    left_ops = noise(keys[2], (PAIRS, SECTORS, M, M), M ** -0.5, 0.25, ((0, 16), (1, 2)), jnp.float32)
    right_ops = noise(keys[3], (PAIRS, SECTORS, M, M), (2 * M * PAIRS) ** -0.5, 0.02734375, ((0, 16), (1, 2)), jnp.float32)
    charges = place_ends(jax.random.randint(keys[4], (PAIRS,), 0, 3), jax.random.fold_in(keys[4], 1), 0, 2).astype(jnp.int32)
    coupling = place_ends((jax.random.randint(keys[5], (SECTORS, 3), 0, 4) < 3).astype(jnp.int32), jax.random.fold_in(keys[5], 1), 0, 1)
    return {"wavefunction": wavefunction, "preconditioner": preconditioner, "left_ops": left_ops, "right_ops": right_ops, "charges": charges, "coupling": coupling}


highest = lax.Precision.HIGHEST

def product(first, second):
    return jnp.dot(first, second, precision=highest, preferred_element_type=jnp.float32)

def sigma_apply(vector, left_ops, right_ops, charges, coupling):
    sectors = vector.shape[0]

    def add_pair(result, pair_index):
        charge_slot = charges[pair_index].astype(jnp.int32)
        for sector in range(sectors):
            target = ((sector + charge_slot - 1) % sectors).astype(jnp.int32)
            allowed = coupling[sector, charge_slot].astype(jnp.float32)
            left_block = left_ops[pair_index, sector]
            right_block = right_ops[pair_index, sector]
            forward = product(product(left_block, vector[sector]), right_block.T)
            source_block = lax.dynamic_index_in_dim(vector, target, 0, keepdims=False)
            backward = product(product(left_block.T, source_block), right_block)
            result = result.at[sector].add(allowed * backward)
            current = lax.dynamic_index_in_dim(result, target, 0, keepdims=False)
            result = lax.dynamic_update_index_in_dim(result, current + allowed * forward, target, 0)
        return (result, None)
    result, unused = lax.scan(add_pair, jnp.zeros_like(vector), jnp.arange(charges.shape[0], dtype=jnp.int32))
    return result

def reference(wavefunction, preconditioner, left_ops, right_ops, charges, coupling):
    first_image = sigma_apply(wavefunction, left_ops, right_ops, charges, coupling)
    norm_sq = jnp.sum(wavefunction * wavefunction)
    correlation = jnp.sum(wavefunction * first_image)
    theta = correlation / norm_sq
    inverse = lax.rsqrt(norm_sq)
    vector = wavefunction * inverse
    image = first_image * inverse
    residual = image - theta * vector
    correction = residual / preconditioner
    along = jnp.sum(vector * correction)
    orthogonal = correction - along * vector
    length_sq = jnp.sum(orthogonal * orthogonal)
    basis = orthogonal * lax.rsqrt(length_sq + 1e-30)
    second_image = sigma_apply(basis, left_ops, right_ops, charges, coupling)
    corner = jnp.sum(basis * second_image)
    cross = jnp.sum(vector * second_image)
    half = (theta - corner) / 2.0
    lowest = (theta + corner) / 2.0 - jnp.sqrt(half * half + cross * cross)
    first_weight = corner - lowest
    second_weight = -cross
    size_norm = jnp.sqrt(first_weight * first_weight + second_weight * second_weight + 1e-30)
    scale = jnp.sqrt(jnp.float32(wavefunction.size))
    factor_one = scale * first_weight / size_norm
    factor_two = scale * second_weight / size_norm
    new_state = factor_one * vector + factor_two * basis
    new_image = factor_one * image + factor_two * second_image
    energies = jnp.stack([theta, lowest]).astype(jnp.float32)
    return (new_state, new_image, energies)
```

```python
import functools
import math

import jax
import jax.numpy as jnp
from jax import lax
from jax.experimental import pallas as pl
from jax.experimental.pallas import tpu as pltpu
from jax.sharding import PartitionSpec as P

F32, BF16 = jnp.float32, jnp.bfloat16
PLANE = 4
LIMIT = 40 * 1024 * 1024


def swap(block, mask):
    return lax.ppermute(block, "pair", [(i, i ^ mask) for i in range(lax.axis_size("pair"))])


def shifted(block, distance):
    size = lax.axis_size("sector")
    return lax.ppermute(block, "sector", [((i - distance) % size, i) for i in range(size)])


def neighbours(block):
    if lax.axis_size("sector") == 2:
        return [shifted(block, 1)]
    return [shifted(block, 1), shifted(block, -1)]


def to_neighbours(blocks):
    if lax.axis_size("sector") == 2:
        return [shifted(blocks[0], 1)]
    return [shifted(blocks[0], -1), shifted(blocks[1], 1)]


def gather_rows(block):
    count, half = lax.axis_size("pair"), block.shape[1] // 2
    column = jnp.concatenate([block] + [swap(block, k) for k in range(PLANE, count, PLANE)], axis=0)
    a, b = column[:, :half], column[:, half:]
    a = jnp.concatenate([a, swap(a, 1)], axis=0)
    b = jnp.concatenate([b, swap(b, 2)], axis=0)
    return [a, b, swap(a, 2), swap(b, 1)]


def piece_slots(count):
    deep = range(0, count, PLANE)
    a = [k + x for x in (0, 1) for k in deep]
    b = [k + y for y in (0, 2) for k in deep]
    return [a, b, [k + 2 for k in a], [k + 1 for k in b]]


def term_slots(count):
    deep = range(0, count, PLANE)
    a = [k + y for y in (0, 2) for k in deep]
    b = [k + x for x in (0, 1) for k in deep]
    return [a, b, [k + 1 for k in a], [k + 2 for k in b]]


def scatter_rows(terms, scalars):
    count = lax.axis_size("pair")
    keep_a, keep_b, send_a, send_b = terms
    a = keep_a + swap(send_a, 1)
    b = keep_b + swap(send_b, 2)
    scalars = scalars + swap(scalars, 1)
    split = a.shape[0] // 2
    a = a[:split] + swap(a[split:], 2)
    b = b[:split] + swap(b[split:], 1)
    scalars = scalars + swap(scalars, 2)
    rows = split // (count // PLANE)
    both = jnp.concatenate([a, b], axis=1)
    total, sums = both[:rows], scalars
    for step in range(1, count // PLANE):
        total = total + swap(both[step * rows : (step + 1) * rows], step * PLANE)
        sums = sums + swap(scalars, step * PLANE)
    return total, sums


def split(value):
    high = value.astype(BF16)
    return high, (value - high.astype(F32)).astype(BF16)


def dot(first, second):
    return jnp.dot(first, second, preferred_element_type=F32)


def dot3(first, second):
    return dot(first[0], second[0]) + dot(first[0], second[1]) + dot(first[1], second[0])


def prepare_kernel(left_ref, right_ref, left_out, left_t_out, right_out, right_t_out):
    for source, plain, turned in ((left_ref, left_out, left_t_out), (right_ref, right_out, right_t_out)):
        value = source[...]
        plain[0], plain[1] = split(value)
        turned[0], turned[1] = split(value.T)


def prepare(left_ops, right_ops):
    pairs, _, m, _ = left_ops.shape
    source = pl.BlockSpec((None, None, m, m), lambda p: (p, 0, 0, 0))
    target = pl.BlockSpec((None, 2, m, m), lambda p: (p, 0, 0, 0))
    return pl.pallas_call(
        prepare_kernel,
        grid=(pairs,),
        in_specs=[source, source],
        out_specs=[target] * 4,
        out_shape=[jax.ShapeDtypeStruct((pairs, 2, m, m), BF16)] * 4,
        compiler_params=pltpu.CompilerParams(vmem_limit_bytes=LIMIT),
        cost_estimate=pl.CostEstimate(flops=pairs * m * m * 1000, bytes_accessed=24 * pairs * m * m, transcendentals=0),
    )(left_ops, right_ops)


def unpack(me, pieces, count, high, low):
    half = pieces[0].shape[1]
    for which, (piece, slots) in enumerate(zip(pieces, piece_slots(count))):
        rows = piece.shape[0] // len(slots)
        columns = pl.ds((which % 2) * half, half)
        for at, slot in enumerate(slots):
            where = pl.multiple_of((me ^ slot) * rows, rows)
            high[pl.ds(where, rows), columns], low[pl.ds(where, rows), columns] = split(
                piece[at * rows : (at + 1) * rows, :]
            )


def pack(me, total, count, pieces, extra=None):
    half = pieces[0].shape[1]
    for which, (piece, slots) in enumerate(zip(pieces, term_slots(count))):
        rows = piece.shape[0] // len(slots)
        columns = pl.ds((which % 2) * half, half)
        for at, slot in enumerate(slots):
            where = pl.multiple_of((me ^ slot) * rows, rows)
            span = slice(at * rows, (at + 1) * rows)
            value = total[pl.ds(where, rows), columns]
            piece[span, :] = value if extra is None else value + extra[which][span, :]


def block_of(charge, sectors):
    return jnp.where(charge == 1, 0, 1 if sectors == 2 else jnp.where(charge == 0, 1, 2))


def forward_kernel(count, sectors, me_ref, charges_ref, coupling_ref, *refs):
    pieces, (left, right_t), refs = refs[:4], refs[4:6], refs[6:]
    blocks = min(sectors, 3)
    outs, (high, low, total) = refs[: 4 * blocks], refs[4 * blocks :]
    pair, me = pl.program_id(0), me_ref[0]

    @pl.when(pair == 0)
    def _():
        unpack(me, pieces, count, high, low)
        total[...] = jnp.zeros_like(total)

    charge = charges_ref[pair]
    allowed = coupling_ref[0, charge].astype(F32)
    inner = dot3((left[0], left[1]), (high[...], low[...])) * allowed
    term = dot3(split(inner), (right_t[0], right_t[1]))
    block = block_of(charge, sectors)
    total[block] = total[block] + term

    @pl.when(pair == pl.num_programs(0) - 1)
    def _():
        for block in range(blocks):
            pack(me, total.at[block], count, outs[4 * block : 4 * block + 4])


def backward_kernel(count, sectors, me_ref, charges_ref, coupling_ref, *refs):
    blocks = min(sectors, 3)
    pieces, refs = refs[: 4 * blocks], refs[4 * blocks :]
    right, left_t, first, refs = refs[0], refs[1], refs[2:6], refs[6:]
    outs, sums, (high, low, total) = refs[:4], refs[4], refs[5:]
    pair, me = pl.program_id(0), me_ref[0]

    @pl.when(pair == 0)
    def _():
        for block in range(blocks):
            unpack(me, pieces[4 * block : 4 * block + 4], count, high.at[block], low.at[block])
        total[...] = jnp.zeros_like(total)

    charge = charges_ref[pair]
    allowed = coupling_ref[0, charge].astype(F32)
    block = block_of(charge, sectors)
    inner = dot3((high[block], low[block]), (right[0], right[1])) * allowed
    total[...] = total[...] + dot3((left_t[0], left_t[1]), split(inner))

    @pl.when(pair == pl.num_programs(0) - 1)
    def _():
        own = high[0].astype(F32) + low[0].astype(F32)
        sums[...] = jnp.full(sums.shape, 2.0 * jnp.sum(own * total[...]), F32)
        pack(me, total, count, outs, first)


def call(kernel, pairs, m, scalars, pieces, ops, extra, outs, scratch):
    whole = pl.BlockSpec(memory_space=pltpu.VMEM)
    op = pl.BlockSpec((None, 2, m, m), lambda p, *_: (p, 0, 0, 0))
    return pl.pallas_call(
        kernel,
        grid_spec=pltpu.PrefetchScalarGridSpec(
            num_scalar_prefetch=3,
            grid=(pairs,),
            in_specs=[whole] * len(pieces) + [op] * len(ops) + [whole] * len(extra),
            out_specs=[whole] * len(outs),
            scratch_shapes=scratch,
        ),
        out_shape=outs,
        compiler_params=pltpu.CompilerParams(vmem_limit_bytes=LIMIT),
        cost_estimate=pl.CostEstimate(flops=12 * pairs * m**3, bytes_accessed=8 * pairs * m * m, transcendentals=0),
    )(*scalars, *pieces, *ops, *extra)


def sigma_apply(block, ops, scalars, extra_sums):
    left, left_t, right, right_t = ops
    pairs, m = left.shape[0], left.shape[2]
    count, sectors = lax.axis_size("pair"), lax.axis_size("sector")
    blocks = min(sectors, 3)
    own = gather_rows(block)
    others = [neighbours(piece) for piece in own]
    others = [[others[q][b] for q in range(4)] for b in range(blocks - 1)]
    shape = jax.ShapeDtypeStruct((m // 2, m // 2), F32)
    tile = jax.ShapeDtypeStruct((8, 128), F32)
    made = call(
        functools.partial(forward_kernel, count, sectors), pairs, m, scalars, own, [left, right_t], [],
        [shape] * (4 * blocks),
        [pltpu.VMEM((m, m), BF16), pltpu.VMEM((m, m), BF16), pltpu.VMEM((blocks, m, m), F32)],
    )
    aimed = [made[4 * b : 4 * b + 4] for b in range(blocks)]
    arrived = [to_neighbours([aimed[b][q] for b in range(1, blocks)]) for q in range(4)]
    *mine, product = call(
        functools.partial(backward_kernel, count, sectors), pairs, m, scalars, own + sum(others, []), [right, left_t],
        aimed[0], [shape] * 4 + [tile],
        [pltpu.VMEM((blocks, m, m), BF16), pltpu.VMEM((blocks, m, m), BF16), pltpu.VMEM((m, m), F32)],
    )
    terms = [sum(arrived[q], mine[q]) for q in range(4)]
    row = lax.broadcasted_iota(jnp.int32, tile.shape, 0)
    sums = jnp.where(row == 0, product, extra_sums)
    if sectors == 2:
        sums = sums + shifted(sums, 1)
    else:
        sums = lax.psum(sums, "sector")
    rows, sums = scatter_rows(terms, sums)
    return rows, sums[:, 0]


def tile_of(values):
    row = lax.broadcasted_iota(jnp.int32, (8, 128), 0)
    tile = jnp.zeros((8, 128), F32)
    for at, value in enumerate(values):
        tile = jnp.where(row == at + 1, value, tile)
    return tile


def per_device(wavefunction, preconditioner, left_ops, right_ops, charges, coupling):
    vector, divisor = wavefunction[0], preconditioner[0]
    ops = prepare(left_ops, right_ops)
    scalars = (lax.axis_index("pair").astype(jnp.int32)[None], charges, coupling)
    image, sums = sigma_apply(vector, ops, scalars, tile_of([jnp.sum(vector * vector)]))
    correlation, norm_sq = sums[0], sums[1]
    theta = correlation / norm_sq
    inverse = lax.rsqrt(norm_sq)
    correction = (image - theta * vector) / divisor
    second, sums = sigma_apply(
        correction, ops, scalars,
        tile_of([jnp.sum(vector * correction), jnp.sum(correction * correction), jnp.sum(image * correction)]),
    )
    along = sums[1] / norm_sq
    length_sq = (sums[2] - along * sums[1]) / norm_sq
    factor = inverse * lax.rsqrt(length_sq + 1e-30)
    corner = factor * factor * (sums[0] - 2.0 * along * sums[3] + along * along * correlation)
    cross = inverse * factor * (sums[3] - along * correlation)
    half = (theta - corner) / 2.0
    lowest = (theta + corner) / 2.0 - jnp.sqrt(half * half + cross * cross)
    first_weight = corner - lowest
    second_weight = -cross
    size_norm = jnp.sqrt(first_weight * first_weight + second_weight * second_weight + 1e-30)
    entries = lax.axis_size("sector") * lax.axis_size("pair") * vector.shape[0] * vector.shape[1]
    scale = jnp.float32(math.sqrt(entries))
    factor_two = scale * second_weight / size_norm * factor
    factor_one = scale * first_weight / size_norm * inverse - factor_two * along
    new_state = factor_one * vector + factor_two * correction
    new_image = factor_one * image + factor_two * second
    return (new_state[None], new_image[None], jnp.stack([theta, lowest]))


def solution(mesh):
    in_specs = (
        P("sector", "pair", None),
        P("sector", "pair", None),
        P("pair", "sector", None, None),
        P("pair", "sector", None, None),
        P("pair"),
        P("sector", None),
    )
    out_specs = (P("sector", "pair", None), P("sector", "pair", None), P())
    return jax.shard_map(
        per_device, mesh=mesh, in_specs=in_specs, out_specs=out_specs, check_vma=False
    )
```

```python
import functools
import math

import jax
import jax.numpy as jnp
from jax import lax
from jax.experimental import pallas as pl
from jax.experimental.pallas import tpu as pltpu
from jax.sharding import PartitionSpec as P

F32, BF16 = jnp.float32, jnp.bfloat16
LIMIT = 12 * 1024 * 1024
X, Y = 1, 2
EDGE = 8


def deep_masks(count):
    bits = [4 << b for b in range((count // 4).bit_length() - 1)]
    return bits[:1] + [bits[0] | bits[1]] + bits[2:] if len(bits) > 1 else bits


def streams(count):
    deep = deep_masks(count)
    return deep + [X, Y], deep[::-1] + [Y, X]


def offsets(masks):
    slots = [0]
    for mask in masks:
        slots = slots + [slot ^ mask for slot in slots]
    return slots


def row_order(count):
    a, b = (offsets(masks) for masks in streams(count))
    middle = count // 2
    return (
        [(s, 0) for s in a[:middle]] + [(s, 1) for s in b[:middle]]
        + [(s, 0) for s in a[middle:]] + [(s, 1) for s in b[middle:]]
    )


def swap(block, mask):
    return lax.ppermute(block, "pair", [(i, i ^ mask) for i in range(lax.axis_size("pair"))])


def shifted(block, distance):
    size = lax.axis_size("sector")
    return lax.ppermute(block, "sector", [((i - distance) % size, i) for i in range(size)])


def neighbours(block):
    if lax.axis_size("sector") == 2:
        return [shifted(block, 1)]
    return [shifted(block, 1), shifted(block, -1)]


def to_neighbours(blocks):
    if lax.axis_size("sector") == 2:
        return [shifted(blocks[0], 1)]
    return [shifted(blocks[0], -1), shifted(blocks[1], 1)]


def over_sectors(tile):
    if lax.axis_size("sector") == 2:
        return [tile, shifted(tile, 1)]
    return [lax.psum(tile, "sector")]


def array(*shape, kind=F32):
    return jax.ShapeDtypeStruct(shape, kind)


def kernel_call(body, outs, *groups, scalars=(), scratch=(), flops=0):
    flat = [value for group in groups for value in group]

    def kernel(*refs):
        refs = list(refs)
        take = lambda n: [refs.pop(0) for _ in range(n)]
        fixed = take(len(scalars))
        inputs = [take(len(group)) for group in groups]
        body(fixed, inputs, take(len(outs)), refs)

    traffic = sum(v.size * v.dtype.itemsize for v in flat)
    return pl.pallas_call(
        kernel,
        in_specs=[pl.BlockSpec(memory_space=pltpu.SMEM)] * len(scalars)
        + [pl.BlockSpec(memory_space=pltpu.VMEM)] * len(flat),
        out_specs=[pl.BlockSpec(memory_space=pltpu.VMEM)] * len(outs),
        out_shape=list(outs),
        scratch_shapes=list(scratch),
        compiler_params=pltpu.CompilerParams(vmem_limit_bytes=LIMIT),
        cost_estimate=pl.CostEstimate(flops=max(flops, traffic), bytes_accessed=traffic, transcendentals=0),
    )(*scalars, *flat)


def split(value):
    high = value.astype(BF16)
    return high, (value - high.astype(F32)).astype(BF16)


def dot(first, second):
    return jnp.dot(first, second, preferred_element_type=F32)


def dot3(first, second):
    return dot(first[0], second[0]) + dot(first[0], second[1]) + dot(first[1], second[0])


def tile_rows(values):
    shape = (EDGE, values[0].shape[1])
    row = lax.broadcasted_iota(jnp.int32, shape, 0)
    tile = jnp.zeros(shape, F32)
    for at, value in enumerate(values):
        tile = jnp.where(row == at, value, tile)
    return tile


def summed(value, width):
    return jnp.broadcast_to(jnp.sum(value, keepdims=True), (1, width))


def prepare(me, left_ops, right_ops, block, count):
    pairs, _, m, _ = left_ops.shape
    rows = m // count // 2
    order = row_order(count)

    def kernel(me_ref, left_ref, right_ref, block_ref, left_out, left_t_out, right_out, right_t_out, edge, held):
        def reorder(value):
            held[...] = value
            parts = []
            for slot, half in order:
                where = pl.multiple_of((me_ref[0] ^ slot) * (2 * rows) + half * rows, rows)
                parts.append(held[pl.ds(where, rows), :])
            return jnp.concatenate(parts, axis=0)

        turned = reorder(reorder(left_ref[...]).T)
        left_t_out[0], left_t_out[1] = split(turned)
        left_out[0], left_out[1] = split(turned.T)
        value = right_ref[...]
        right_out[0], right_out[1] = split(value)
        right_t_out[0], right_t_out[1] = split(value.T)
        edge[...] = tile_rows([jnp.zeros((1, m), F32), summed(block_ref[...] * block_ref[...], m)])

    source = pl.BlockSpec((None, None, m, m), lambda p, *_: (p, 0, 0, 0))
    target = pl.BlockSpec((None, 2, m, m), lambda p, *_: (p, 0, 0, 0))
    whole = pl.BlockSpec(memory_space=pltpu.VMEM)
    return pl.pallas_call(
        kernel,
        grid_spec=pltpu.PrefetchScalarGridSpec(
            num_scalar_prefetch=1,
            grid=(pairs,),
            in_specs=[source, source, whole],
            out_specs=[target] * 4 + [whole],
            scratch_shapes=[pltpu.VMEM((m, m), F32)],
        ),
        out_shape=[array(pairs, 2, m, m, kind=BF16)] * 4 + [array(EDGE, m)],
        compiler_params=pltpu.CompilerParams(vmem_limit_bytes=2 * LIMIT),
        cost_estimate=pl.CostEstimate(flops=pairs * m * m * 1500, bytes_accessed=24 * pairs * m * m, transcendentals=0),
    )(me, left_ops, right_ops, block)


def block_of(charge, sectors):
    return jnp.where(charge == 1, 0, 1 if sectors == 2 else jnp.where(charge == 0, 1, 2))


def double(a, b, masks_a, masks_b):
    for mask_a, mask_b in zip(masks_a, masks_b):
        more_a, more_b = swap(a, mask_a), swap(b, mask_b)
        rows, m = a.shape

        def body(_, inputs, outs, scratch):
            for (low, high), out in zip(inputs, outs):
                out[:rows, :] = low[...]
                out[rows:, :] = high[...]

        a, b = kernel_call(body, [array(2 * rows, m)] * 2, [a, more_a], [b, more_b])
    return a, b


def sigma_apply(column_a, column_b, ops, scalars, edge):
    left, left_t, right, right_t = ops
    pairs, m = left.shape[0], left.shape[2]
    count, sectors = lax.axis_size("pair"), lax.axis_size("sector")
    blocks = min(sectors, 3)
    half, quarter, eighth = m // 2, m // 4, m // 8
    rows_of = array(half, m)
    made = array(pairs, 2, half, m, kind=BF16)
    held = pltpu.VMEM((blocks, 2, half, m), BF16)
    cost = 6 * half * m * m * pairs

    def hold(scratch, groups):
        for block, group in enumerate(groups):
            at = 0
            for ref in group:
                size = ref.shape[0]
                scratch[block, 0, at : at + size, :], scratch[block, 1, at : at + size, :] = split(ref[...])
                at += size

    def gains(fixed, pair):
        charge = fixed[0][pair]
        return block_of(charge, sectors), fixed[1][0, charge].astype(F32)

    def parts(ref, *index):
        return ref[index[0], 0], ref[index[0], 1]

    more_a, more_b = swap(column_a, X), swap(column_b, Y)

    def join(_, inputs, outs, scratch):
        both, a, b = outs
        for at, (low, high), out in ((0, inputs[0], a), (quarter, inputs[1], b)):
            out[:eighth, :] = low[...]
            out[eighth:, :] = high[...]
            both[at : at + eighth, :] = low[...]
            both[at + eighth : at + quarter, :] = high[...]

    early, a, b = kernel_call(
        join, [rows_of, array(quarter, m), array(quarter, m)], [column_a, more_a], [column_b, more_b]
    )
    late = [swap(a, Y), swap(b, X)]
    early_others = neighbours(early)

    def first_inner(fixed, inputs, outs, scratch):
        (own, *others), rights, rights_t = inputs
        hold(scratch[0], [[own]] + [[other] for other in others])
        for pair in range(pairs):
            block, allowed = gains(fixed, pair)
            forward = dot3(parts(scratch[0], 0), parts(rights_t[0], pair)) * allowed
            outs[0][pair, 0], outs[0][pair, 1] = split(forward)
            backward = dot3((scratch[0][block, 0], scratch[0][block, 1]), parts(rights[0], pair)) * allowed
            outs[1][pair, 0], outs[1][pair, 1] = split(backward)

    early_z, early_y = kernel_call(
        first_inner, [made] * 2, [early] + early_others, [right], [right_t],
        scalars=scalars, scratch=[held], flops=2 * cost,
    )
    late_others = [neighbours(piece) for piece in late]
    late_others = [[late_others[q][b] for q in range(2)] for b in range(blocks - 1)]

    def outer(ref, pair, at, first, second):
        rows = slice(at, at + half)
        total = dot3((ref[pair, 0, rows, :half], ref[pair, 1, rows, :half]), first)
        return total + dot3((ref[pair, 0, rows, half:], ref[pair, 1, rows, half:]), second)

    def forward_late(fixed, inputs, outs, scratch):
        own, (early_ref,), (rights_t,), (lefts,) = inputs
        z_out, total = outs[0], scratch[1]
        hold(scratch[0], [own])
        total[...] = jnp.zeros_like(total)
        for pair in range(pairs):
            block, allowed = gains(fixed, pair)
            inner = split(dot3(parts(scratch[0], 0), parts(rights_t, pair)) * allowed)
            z_out[pair, 0], z_out[pair, 1] = inner
            total[block] = total[block] + outer(lefts, pair, half, parts(early_ref, pair), inner)
        for block in range(blocks):
            outs[1 + block][...] = total[block]

    late_z, own_sent, *aimed = kernel_call(
        forward_late, [made] + [rows_of] * blocks, late, [early_z], [right_t], [left],
        scalars=scalars, scratch=[held, pltpu.VMEM((blocks, half, m), F32)], flops=3 * cost,
    )
    aimed_sent = to_neighbours(aimed)

    def backward_late(fixed, inputs, outs, scratch):
        groups, (early_ref,), (rights,), (lefts_t,), (base,) = inputs
        y_out, sent, product = outs
        hold(scratch[0], [groups[2 * block : 2 * block + 2] for block in range(blocks)])
        total = jnp.zeros((half, m), F32)
        for pair in range(pairs):
            block, allowed = gains(fixed, pair)
            inner = split(dot3((scratch[0][block, 0], scratch[0][block, 1]), parts(rights, pair)) * allowed)
            y_out[pair, 0], y_out[pair, 1] = inner
            total = total + outer(lefts_t, pair, half, parts(early_ref, pair), inner)
        sent[...] = total + base[...]
        own = jnp.concatenate([groups[0][...], groups[1][...]], axis=0)
        product[...] = jnp.broadcast_to(summed(own * total, m), (EDGE, m))

    late_y, own_sent, product = kernel_call(
        backward_late, [made, rows_of, array(EDGE, m)], late + sum(late_others, []), [early_y], [right], [left_t],
        [own_sent], scalars=scalars, scratch=[held], flops=3 * cost,
    )

    def add_sent(_, inputs, outs, scratch):
        value = sum(ref[...] for ref in inputs[0])
        outs[0][...] = value[:quarter]
        outs[1][...] = value[quarter:]

    sent_a, sent_b = kernel_call(add_sent, [array(quarter, m)] * 2, [own_sent] + aimed_sent)
    got_a, got_b = swap(sent_a, Y), swap(sent_b, X)

    def keep(fixed, inputs, outs, scratch):
        (z0, z1), (y0, y1), (lefts,), (lefts_t,), (own, product_ref, edge_ref) = inputs
        total = scratch[0]
        total[...] = jnp.zeros_like(total)
        back = jnp.zeros((half, m), F32)
        for pair in range(pairs):
            block, _ = gains(fixed, pair)
            total[block] = total[block] + outer(lefts, pair, 0, parts(z0, pair), parts(z1, pair))
        for block in range(1, blocks):
            outs[1 + block][...] = total[block]
        for pair in range(pairs):
            back = back + outer(lefts_t, pair, 0, parts(y0, pair), parts(y1, pair))
        outs[0][...] = total[0] + back
        product_sum = 2.0 * (summed(own[...] * back, m) + product_ref[:1, :])
        row = lax.broadcasted_iota(jnp.int32, (EDGE, m), 0)
        outs[1][...] = jnp.where(row == 0, product_sum, edge_ref[...])

    own_kept, edge, *aimed = kernel_call(
        keep, [rows_of, array(EDGE, m)] + [rows_of] * (blocks - 1), [early_z, late_z], [early_y, late_y], [left],
        [left_t], [early, product, edge],
        scalars=scalars, scratch=[pltpu.VMEM((blocks, half, m), F32)], flops=4 * cost,
    )
    aimed_kept = to_neighbours(aimed)
    edges = over_sectors(edge)

    def first_sum(_, inputs, outs, scratch):
        kept, (a_ref, b_ref), edge_refs = inputs
        value = sum(ref[...] for ref in kept)
        edge_sum = sum(ref[...] for ref in edge_refs)
        a_value, b_value = value[:quarter] + a_ref[...], value[quarter:] + b_ref[...]
        for (stay, go), total in ((outs[:2], a_value), (outs[2:4], b_value)):
            stay[...] = total[:eighth]
            go[:eighth, :] = total[eighth:]
            go[eighth:, :] = edge_sum
        outs[4][...] = edge_sum

    stay_a, go_a, stay_b, go_b, edge = kernel_call(
        first_sum, [array(eighth, m), array(eighth + EDGE, m)] * 2 + [array(EDGE, m)],
        [own_kept] + aimed_kept, [got_a, got_b], edges,
    )
    got_a, got_b, corner = swap(go_a, X), swap(go_b, Y), swap(edge, X | Y)

    def second_sum(_, inputs, outs, scratch):
        (a_stay, a_got), (b_stay, b_got), (edge_ref, corner_ref) = inputs
        outs[0][:eighth, :] = a_stay[...] + a_got[:eighth, :]
        outs[0][eighth:, :] = edge_ref[...] + a_got[eighth:, :] + b_got[eighth:, :] + corner_ref[...]
        outs[1][...] = b_stay[...] + b_got[:eighth, :]

    return kernel_call(
        second_sum, [array(eighth + EDGE, m), array(eighth, m)], [stay_a, got_a], [stay_b, got_b], [edge, corner]
    )


def turned(value, slots, mask, rows):
    parts = [value[slots.index(slot ^ mask) * rows :][:rows] for slot in slots]
    rest = value[len(slots) * rows :]
    return jnp.concatenate(parts + ([rest] if rest.shape[0] else []), axis=0)


def per_device(wavefunction, preconditioner, left_ops, right_ops, charges, coupling):
    vector, divisor = wavefunction[0], preconditioner[0]
    count = lax.axis_size("pair")
    deep = deep_masks(count)
    rows, m = vector.shape[0] // 2, vector.shape[1]
    tall = rows * (count // 4)
    me = lax.axis_index("pair").astype(jnp.int32)[None]
    *ops, edge = prepare(me, left_ops, right_ops, vector, count)
    scalars = (charges, coupling)
    vector_a, vector_b = double(vector[:rows], vector[rows:], deep, deep[::-1])
    divisor, _ = lax.optimization_barrier((divisor, vector_a))
    divisor_a, divisor_b = double(divisor[:rows], divisor[rows:], deep, deep[::-1])

    image_a, image_b = sigma_apply(vector_a, vector_b, ops, scalars, edge)
    slots_a, slots_b = offsets(deep), offsets(deep[::-1])
    for mask_a, mask_b in zip(deep[:0:-1], deep[:-1]):

        def add_columns(_, inputs, outs, scratch):
            (a_ref, a_got), (b_ref, b_got) = inputs
            outs[0][...] = a_ref[...] + turned(a_got[...], slots_a, mask_a, rows)
            outs[1][...] = b_ref[...] + turned(b_got[...], slots_b, mask_b, rows)

        image_a, image_b = kernel_call(
            add_columns, [array(*image_a.shape), array(*image_b.shape)],
            [image_a, swap(image_a, mask_a)], [image_b, swap(image_b, mask_b)],
        )

    last_a, last_b = deep[0], deep[-1]

    def correct(_, inputs, outs, scratch):
        (a0, a1), (b0, b1), (wa, wb), (pa, pb) = inputs
        correction_a, correction_b, image_own, sums_out, edge_out = outs
        total_a = a0[...] + turned(a1[...], slots_a, last_a, rows)
        total_b = b0[...] + turned(b1[...], slots_b, last_b, rows)
        sums = total_a[tall:]
        theta = sums[0:1, :] / sums[1:2, :]
        ca = (total_a[:tall] - theta * wa[...]) / pa[...]
        cb = (total_b - theta * wb[...]) / pb[...]
        correction_a[...] = ca
        correction_b[...] = cb
        image_own[:rows, :] = total_a[:rows]
        image_own[rows:, :] = total_b[:rows]
        sums_out[...] = sums

        def inner(first, second):
            return summed(first[0] * second[0], m) + summed(first[1] * second[1], m)

        own_w, own_c = (wa[:rows, :], wb[:rows, :]), (ca[:rows], cb[:rows])
        own_a = (total_a[:rows], total_b[:rows])
        edge_out[...] = tile_rows(
            [jnp.zeros((1, m), F32), inner(own_w, own_c), inner(own_c, own_c), inner(own_a, own_c)]
        )

    ca, cb, image_own, sums, edge = kernel_call(
        correct, [array(tall, m), array(tall, m), array(2 * rows, m), array(EDGE, m), array(EDGE, m)],
        [image_a, swap(image_a, last_a)], [image_b, swap(image_b, last_b)], [vector_a, vector_b],
        [divisor_a, divisor_b],
    )
    own_c = (ca, cb)
    second_a, second_b = sigma_apply(ca, cb, ops, scalars, edge)

    for mask_a, mask_b in zip(deep[::-1], deep):
        size = second_b.shape[0] // 2

        def cut(_, inputs, outs, scratch):
            a_ref, b_ref = inputs[0]
            outs[0][...] = a_ref[size:, :]
            outs[1][...] = b_ref[size:, :]

        def meet(_, inputs, outs, scratch):
            (a_ref, a_got), (b_ref, b_got) = inputs
            outs[0][:size, :] = a_ref[:size, :] + a_got[:size, :]
            outs[0][size:, :] = a_ref[2 * size :, :] + a_got[size:, :]
            outs[1][...] = b_ref[:size, :] + b_got[...]

        go_a, go_b = kernel_call(cut, [array(size + EDGE, m), array(size, m)], [second_a, second_b])
        second_a, second_b = kernel_call(
            meet, [array(size + EDGE, m), array(size, m)],
            [second_a, swap(go_a, mask_a)], [second_b, swap(go_b, mask_b)],
        )

    scale = math.sqrt(lax.axis_size("sector") * count * vector.shape[0] * m)

    def finish(_, inputs, outs, scratch):
        (a_ref, b_ref), (vector_ref, image_ref, ca_ref, cb_ref), (first_ref,) = inputs
        sums = a_ref[rows:, :]
        correlation, norm_sq = first_ref[0:1, :], first_ref[1:2, :]
        theta = correlation / norm_sq
        inverse = lax.rsqrt(norm_sq)
        along = sums[1:2] / norm_sq
        length_sq = (sums[2:3] - along * sums[1:2]) / norm_sq
        factor = inverse * lax.rsqrt(length_sq + 1e-30)
        corner = factor * factor * (sums[0:1] - 2.0 * along * sums[3:4] + along * along * correlation)
        cross = inverse * factor * (sums[3:4] - along * correlation)
        spread = (theta - corner) / 2.0
        lowest = (theta + corner) / 2.0 - jnp.sqrt(spread * spread + cross * cross)
        first_weight = corner - lowest
        second_weight = -cross
        size_norm = jnp.sqrt(first_weight * first_weight + second_weight * second_weight + 1e-30)
        factor_two = scale * second_weight / size_norm * factor
        factor_one = scale * first_weight / size_norm * inverse - factor_two * along
        for at, c_ref, s_ref in ((0, ca_ref, a_ref), (rows, cb_ref, b_ref)):
            span = slice(at, at + rows)
            outs[0][span, :] = factor_one * vector_ref[span, :] + factor_two * c_ref[:rows, :]
            outs[1][span, :] = factor_one * image_ref[span, :] + factor_two * s_ref[:rows, :]
        row = lax.broadcasted_iota(jnp.int32, (EDGE, m), 1)
        outs[2][...] = jnp.where(row == 0, theta, lowest)

    state, image, energies = kernel_call(
        finish, [array(2 * rows, m), array(2 * rows, m), array(EDGE, m)], [second_a, second_b],
        [vector, image_own, own_c[0], own_c[1]], [sums],
    )
    return (state[None], image[None], energies[0, :2])


def solution(mesh):
    in_specs = (
        P("sector", "pair", None),
        P("sector", "pair", None),
        P("pair", "sector", None, None),
        P("pair", "sector", None, None),
        P("pair"),
        P("sector", None),
    )
    out_specs = (P("sector", "pair", None), P("sector", "pair", None), P())
    return jax.shard_map(
        per_device, mesh=mesh, in_specs=in_specs, out_specs=out_specs, check_vma=False
    )
```

```python
import math

import jax
import jax.numpy as jnp
from jax import lax
from jax.experimental import pallas as pl
from jax.experimental.pallas import tpu as pltpu
from jax.sharding import PartitionSpec as P


F32, BF16 = jnp.float32, jnp.bfloat16
LIMIT = 12 * 1024 * 1024
X, Y = 1, 2
EDGE = 8


def deep_masks(count):
    bits = [4 << b for b in range((count // 4).bit_length() - 1)]
    return bits[:1] + [bits[0] | bits[1]] + bits[2:] if len(bits) > 1 else bits


def streams(count):
    deep = deep_masks(count)
    return deep + [X, Y], deep + [Y, X]


def offsets(masks):
    slots = [0]
    for mask in masks:
        slots = slots + [slot ^ mask for slot in slots]
    return slots


def row_order(count):
    a, b = (offsets(masks) for masks in streams(count))
    middle = count // 2
    return (
        [(s, 0) for s in a[:middle]] + [(s, 1) for s in b[:middle]]
        + [(s, 0) for s in a[middle:]] + [(s, 1) for s in b[middle:]]
    )


def swap(block, mask):
    return lax.ppermute(block, "pair", [(i, i ^ mask) for i in range(lax.axis_size("pair"))])


def shifted(block, distance):
    size = lax.axis_size("sector")
    return lax.ppermute(block, "sector", [((i - distance) % size, i) for i in range(size)])


def neighbours(block):
    if lax.axis_size("sector") == 2:
        return [shifted(block, 1)]
    return [shifted(block, 1), shifted(block, -1)]


def to_neighbours(blocks):
    if lax.axis_size("sector") == 2:
        return [shifted(blocks[0], 1)]
    return [shifted(blocks[0], -1), shifted(blocks[1], 1)]


def over_sectors(tile):
    if lax.axis_size("sector") == 2:
        return [tile, shifted(tile, 1)]
    return [lax.psum(tile, "sector")]


def array(*shape, kind=F32):
    return jax.ShapeDtypeStruct(shape, kind)


def kernel_call(body, outs, *groups, scalars=(), scratch=(), flops=0):
    flat = [value for group in groups for value in group]

    def kernel(*refs):
        refs = list(refs)
        take = lambda n: [refs.pop(0) for _ in range(n)]
        fixed = take(len(scalars))
        inputs = [take(len(group)) for group in groups]
        body(fixed, inputs, take(len(outs)), refs)

    traffic = sum(v.size * v.dtype.itemsize for v in flat)
    return pl.pallas_call(
        kernel,
        in_specs=[pl.BlockSpec(memory_space=pltpu.SMEM)] * len(scalars)
        + [pl.BlockSpec(memory_space=pltpu.VMEM)] * len(flat),
        out_specs=[pl.BlockSpec(memory_space=pltpu.VMEM)] * len(outs),
        out_shape=list(outs),
        scratch_shapes=list(scratch),
        compiler_params=pltpu.CompilerParams(vmem_limit_bytes=LIMIT),
        cost_estimate=pl.CostEstimate(flops=max(flops, traffic), bytes_accessed=traffic, transcendentals=0),
    )(*scalars, *flat)


def split(value):
    high = value.astype(BF16)
    return high, (value - high.astype(F32)).astype(BF16)


def dot(first, second):
    return jnp.dot(first, second, preferred_element_type=F32)


def dot3(first, second):
    return dot(first[0], second[0]) + dot(first[0], second[1]) + dot(first[1], second[0])


def tile_rows(values):
    shape = (EDGE, values[0].shape[1])
    row = lax.broadcasted_iota(jnp.int32, shape, 0)
    tile = jnp.zeros(shape, F32)
    for at, value in enumerate(values):
        tile = jnp.where(row == at, value, tile)
    return tile


def summed(value, width):
    return jnp.broadcast_to(jnp.sum(value, keepdims=True), (1, width))


def prepare(me, left_ops, right_ops, block, count):
    pairs, _, m, _ = left_ops.shape
    rows = m // count // 2
    order = row_order(count)

    def kernel(me_ref, left_ref, right_ref, block_ref, left_out, left_t_out, right_out, right_t_out, edge, held):
        def reorder(value):
            held[...] = value
            parts = []
            for slot, half in order:
                where = pl.multiple_of((me_ref[0] ^ slot) * (2 * rows) + half * rows, rows)
                parts.append(held[pl.ds(where, rows), :])
            return jnp.concatenate(parts, axis=0)

        turned = reorder(reorder(left_ref[...]).T)
        left_t_out[0], left_t_out[1] = split(turned)
        left_out[0], left_out[1] = split(turned.T)
        value = right_ref[...]
        right_out[0], right_out[1] = split(value)
        right_t_out[0], right_t_out[1] = split(value.T)
        edge[...] = tile_rows([jnp.zeros((1, m), F32), summed(block_ref[...] * block_ref[...], m)])

    source = pl.BlockSpec((None, None, m, m), lambda p, *_: (p, 0, 0, 0))
    target = pl.BlockSpec((None, 2, m, m), lambda p, *_: (p, 0, 0, 0))
    whole = pl.BlockSpec(memory_space=pltpu.VMEM)
    return pl.pallas_call(
        kernel,
        grid_spec=pltpu.PrefetchScalarGridSpec(
            num_scalar_prefetch=1,
            grid=(pairs,),
            in_specs=[source, source, whole],
            out_specs=[target] * 4 + [whole],
            scratch_shapes=[pltpu.VMEM((m, m), F32)],
        ),
        out_shape=[array(pairs, 2, m, m, kind=BF16)] * 4 + [array(EDGE, m)],
        compiler_params=pltpu.CompilerParams(vmem_limit_bytes=10 * LIMIT // 3),
        cost_estimate=pl.CostEstimate(flops=pairs * m * m * 1500, bytes_accessed=24 * pairs * m * m, transcendentals=0),
    )(me, left_ops, right_ops, block)


def block_of(charge, sectors):
    return jnp.where(charge == 1, 0, 1 if sectors == 2 else jnp.where(charge == 0, 1, 2))


def double(block, masks):
    for mask in masks:
        more = swap(block, mask)
        rows, m = block.shape[0] // 2, block.shape[1]

        def meet_column(_, inputs, outs, scratch):
            (low, high), (out,) = inputs[0], outs
            for part in (0, 1):
                span = slice(part * rows, (part + 1) * rows)
                out[2 * part * rows : (2 * part + 1) * rows, :] = low[span, :]
                out[(2 * part + 1) * rows : (2 * part + 2) * rows, :] = high[span, :]

        (block,) = kernel_call(meet_column, [array(4 * rows, m)], [block, more])
    return block


def sigma_apply(column_a, column_b, ops, scalars, edge):
    left, left_t, right, right_t = ops
    pairs, m = left.shape[0], left.shape[2]
    sectors = lax.axis_size("sector")
    blocks = min(sectors, 3)
    half, quarter, eighth = m // 2, m // 4, m // 8
    rows_of = array(half, m)
    made = array(pairs, 2, half, m, kind=BF16)
    held = pltpu.VMEM((blocks, 2, half, m), BF16)
    cost = 6 * half * m * m * pairs

    def hold(scratch, groups):
        for block, group in enumerate(groups):
            at = 0
            for ref in group:
                size = ref.shape[0]
                scratch[block, 0, at : at + size, :], scratch[block, 1, at : at + size, :] = split(ref[...])
                at += size

    def gains(fixed, pair):
        charge = fixed[0][pair]
        return block_of(charge, sectors), fixed[1][0, charge].astype(F32)

    def parts(ref, *index):
        return ref[index[0], 0], ref[index[0], 1]

    more_a, more_b = swap(column_a, X), swap(column_b, Y)

    def join(_, inputs, outs, scratch):
        both, a, b = outs
        for at, (low, high), out in ((0, inputs[0], a), (quarter, inputs[1], b)):
            out[:eighth, :] = low[...]
            out[eighth:, :] = high[...]
            both[at : at + eighth, :] = low[...]
            both[at + eighth : at + quarter, :] = high[...]

    early, a, b = kernel_call(
        join, [rows_of, array(quarter, m), array(quarter, m)], [column_a, more_a], [column_b, more_b]
    )
    early_others = neighbours(early)
    late = [swap(a, Y), swap(b, X)]

    def first_inner(fixed, inputs, outs, scratch):
        (own, *others), rights, rights_t = inputs
        hold(scratch[0], [[own]] + [[other] for other in others])
        for pair in range(pairs):
            block, allowed = gains(fixed, pair)
            forward = dot3(parts(scratch[0], 0), parts(rights_t[0], pair)) * allowed
            outs[0][pair, 0], outs[0][pair, 1] = split(forward)
            backward = dot3((scratch[0][block, 0], scratch[0][block, 1]), parts(rights[0], pair)) * allowed
            outs[1][pair, 0], outs[1][pair, 1] = split(backward)

    early_z, early_y = kernel_call(
        first_inner, [made] * 2, [early] + early_others, [right], [right_t],
        scalars=scalars, scratch=[held], flops=2 * cost,
    )
    late_others = [neighbours(piece) for piece in late]
    late_others = [[late_others[q][b] for q in range(2)] for b in range(blocks - 1)]

    def outer(ref, pair, at, first, second):
        rows = slice(at, at + half)
        total = dot3((ref[pair, 0, rows, :half], ref[pair, 1, rows, :half]), first)
        return total + dot3((ref[pair, 0, rows, half:], ref[pair, 1, rows, half:]), second)

    def forward_late(fixed, inputs, outs, scratch):
        own, (early_ref,), (rights_t,), (lefts,) = inputs
        z_out, total = outs[0], scratch[1]
        hold(scratch[0], [own])
        total[...] = jnp.zeros_like(total)
        for pair in range(pairs):
            block, allowed = gains(fixed, pair)
            inner = split(dot3(parts(scratch[0], 0), parts(rights_t, pair)) * allowed)
            z_out[pair, 0], z_out[pair, 1] = inner
            total[block] = total[block] + outer(lefts, pair, half, parts(early_ref, pair), inner)
        for block in range(blocks):
            outs[1 + block][...] = total[block]

    late_z, own_sent, *aimed = kernel_call(
        forward_late, [made] + [rows_of] * blocks, late, [early_z], [right_t], [left],
        scalars=scalars, scratch=[held, pltpu.VMEM((blocks, half, m), F32)], flops=3 * cost,
    )
    aimed_sent = to_neighbours(aimed)

    def backward_late(fixed, inputs, outs, scratch):
        groups, (early_ref,), (rights,), (lefts_t,), (base,) = inputs
        y_out, sent, product = outs
        hold(scratch[0], [groups[2 * block : 2 * block + 2] for block in range(blocks)])
        total = jnp.zeros((half, m), F32)
        for pair in range(pairs):
            block, allowed = gains(fixed, pair)
            inner = split(dot3((scratch[0][block, 0], scratch[0][block, 1]), parts(rights, pair)) * allowed)
            y_out[pair, 0], y_out[pair, 1] = inner
            total = total + outer(lefts_t, pair, half, parts(early_ref, pair), inner)
        sent[...] = total + base[...]
        own = jnp.concatenate([groups[0][...], groups[1][...]], axis=0)
        product[...] = jnp.broadcast_to(summed(own * total, m), (EDGE, m))

    late_y, own_sent, product = kernel_call(
        backward_late, [made, rows_of, array(EDGE, m)], late + sum(late_others, []), [early_y], [right], [left_t],
        [own_sent], scalars=scalars, scratch=[held], flops=3 * cost,
    )

    def add_sent(_, inputs, outs, scratch):
        value = sum(ref[...] for ref in inputs[0])
        outs[0][...] = value[:quarter]
        outs[1][...] = value[quarter:]

    sent_a, sent_b = kernel_call(add_sent, [array(quarter, m)] * 2, [own_sent] + aimed_sent)
    got_a, got_b = swap(sent_a, Y), swap(sent_b, X)

    def keep(fixed, inputs, outs, scratch):
        (z0, z1), (y0, y1), (lefts,), (lefts_t,), (own, product_ref, edge_ref) = inputs
        total = scratch[0]
        total[...] = jnp.zeros_like(total)
        back = jnp.zeros((half, m), F32)
        for pair in range(pairs):
            block, _ = gains(fixed, pair)
            total[block] = total[block] + outer(lefts, pair, 0, parts(z0, pair), parts(z1, pair))
        for block in range(1, blocks):
            outs[1 + block][...] = total[block]
        for pair in range(pairs):
            back = back + outer(lefts_t, pair, 0, parts(y0, pair), parts(y1, pair))
        outs[0][...] = total[0] + back
        product_sum = 2.0 * (summed(own[...] * back, m) + product_ref[:1, :])
        row = lax.broadcasted_iota(jnp.int32, (EDGE, m), 0)
        outs[1][...] = jnp.where(row == 0, product_sum, edge_ref[...])

    own_kept, edge, *aimed = kernel_call(
        keep, [rows_of, array(EDGE, m)] + [rows_of] * (blocks - 1), [early_z, late_z], [early_y, late_y], [left],
        [left_t], [early, product, edge],
        scalars=scalars, scratch=[pltpu.VMEM((blocks, half, m), F32)], flops=4 * cost,
    )
    aimed_kept = to_neighbours(aimed)
    edges = over_sectors(edge)

    def first_sum(_, inputs, outs, scratch):
        kept, (a_ref, b_ref), edge_refs = inputs
        value = sum(ref[...] for ref in kept)
        edge_sum = sum(ref[...] for ref in edge_refs)
        a_value, b_value = value[:quarter] + a_ref[...], value[quarter:] + b_ref[...]
        for (stay, go), total in ((outs[:2], a_value), (outs[2:4], b_value)):
            stay[...] = total[:eighth]
            go[:eighth, :] = total[eighth:]
            go[eighth:, :] = edge_sum
        outs[4][...] = edge_sum

    stay_a, go_a, stay_b, go_b, edge = kernel_call(
        first_sum, [array(eighth, m), array(eighth + EDGE, m)] * 2 + [array(EDGE, m)],
        [own_kept] + aimed_kept, [got_a, got_b], edges,
    )
    got_a, got_b, corner = swap(go_a, X), swap(go_b, Y), swap(edge, X | Y)

    def second_sum(_, inputs, outs, scratch):
        (a_stay, a_got), (b_stay, b_got), (edge_ref, corner_ref) = inputs
        outs[0][:eighth, :] = a_stay[...] + a_got[:eighth, :]
        outs[0][eighth:quarter, :] = b_stay[...] + b_got[:eighth, :]
        outs[0][quarter:, :] = edge_ref[...] + a_got[eighth:, :] + b_got[eighth:, :] + corner_ref[...]

    return kernel_call(second_sum, [array(quarter + EDGE, m)], [stay_a, got_a], [stay_b, got_b], [edge, corner])[0]


def turned(value, slots, mask, rows):
    size = len(slots) * rows
    parts = [
        value[part * size + slots.index(slot ^ mask) * rows :][:rows] for part in (0, 1) for slot in slots
    ]
    return jnp.concatenate(parts + [value[2 * size :]], axis=0)


def per_device(wavefunction, preconditioner, left_ops, right_ops, charges, coupling):
    vector, divisor = wavefunction[0], preconditioner[0]
    count = lax.axis_size("pair")
    deep = deep_masks(count)
    slots = offsets(deep)
    rows, m = vector.shape[0] // 2, vector.shape[1]
    tall = rows * len(slots)
    me = lax.axis_index("pair").astype(jnp.int32)[None]
    scalars = (charges, coupling)
    *ops, edge = prepare(me, left_ops, right_ops, vector, count)
    column = double(vector, deep)
    divisor = double(divisor, deep)

    def part(_, inputs, outs, scratch):
        outs[0][...] = inputs[0][0][:tall, :]
        outs[1][...] = inputs[0][0][tall:, :]

    vector_a, vector_b = kernel_call(part, [array(tall, m)] * 2, [column])
    image = sigma_apply(vector_a, vector_b, ops, scalars, edge)
    for mask in deep[:0:-1]:

        def add_columns(_, inputs, outs, scratch):
            own, got = inputs[0]
            outs[0][...] = own[...] + turned(got[...], slots, mask, rows)

        (image,) = kernel_call(add_columns, [array(*image.shape)], [image, swap(image, mask)])

    def correct(_, inputs, outs, scratch):
        own, got, w_ref, p_ref = inputs[0]
        correction_a, correction_b, image_own, sums_out, edge_out = outs
        total = own[...] + turned(got[...], slots, deep[0], rows)
        sums = total[2 * tall :]
        theta = sums[0:1, :] / sums[1:2, :]
        c = (total[: 2 * tall] - theta * w_ref[...]) / p_ref[...]
        correction_a[...] = c[:tall]
        correction_b[...] = c[tall:]
        sums_out[...] = sums

        def owned(value):
            return jnp.concatenate([value[:rows], value[tall : tall + rows]], axis=0)

        own_w, own_c, own_a = owned(w_ref[...]), owned(c), owned(total)
        image_own[...] = own_a
        edge_out[...] = tile_rows(
            [jnp.zeros((1, m), F32), summed(own_w * own_c, m), summed(own_c * own_c, m), summed(own_a * own_c, m)]
        )

    ca, cb, image_own, sums, edge = kernel_call(
        correct, [array(tall, m), array(tall, m), array(2 * rows, m), array(EDGE, m), array(EDGE, m)],
        [image, swap(image, deep[0]), column, divisor],
    )
    own_c = (ca, cb)
    second = sigma_apply(ca, cb, ops, scalars, edge)

    for mask in deep[::-1]:
        size = (second.shape[0] - EDGE) // 4

        def cut(_, inputs, outs, scratch):
            ref, out = inputs[0][0], outs[0]
            out[:size, :] = ref[size : 2 * size, :]
            out[size:, :] = ref[3 * size :, :]

        def meet(_, inputs, outs, scratch):
            (ref, got), out = inputs[0], outs[0]
            out[:size, :] = ref[:size, :] + got[:size, :]
            out[size : 2 * size, :] = ref[2 * size : 3 * size, :] + got[size : 2 * size, :]
            out[2 * size :, :] = ref[4 * size :, :] + got[2 * size :, :]

        shape = [array(2 * size + EDGE, m)]
        (go,) = kernel_call(cut, shape, [second])
        (second,) = kernel_call(meet, shape, [second, swap(go, mask)])

    scale = math.sqrt(lax.axis_size("sector") * count * vector.shape[0] * m)

    def finish(_, inputs, outs, scratch):
        (second_ref,), (vector_ref, image_ref, ca_ref, cb_ref), (first_ref,) = inputs
        sums = second_ref[2 * rows :, :]
        correlation, norm_sq = first_ref[0:1, :], first_ref[1:2, :]
        theta = correlation / norm_sq
        inverse = lax.rsqrt(norm_sq)
        along = sums[1:2] / norm_sq
        length_sq = (sums[2:3] - along * sums[1:2]) / norm_sq
        factor = inverse * lax.rsqrt(length_sq + 1e-30)
        corner = factor * factor * (sums[0:1] - 2.0 * along * sums[3:4] + along * along * correlation)
        cross = inverse * factor * (sums[3:4] - along * correlation)
        spread = (theta - corner) / 2.0
        lowest = (theta + corner) / 2.0 - jnp.sqrt(spread * spread + cross * cross)
        first_weight = corner - lowest
        second_weight = -cross
        size_norm = jnp.sqrt(first_weight * first_weight + second_weight * second_weight + 1e-30)
        factor_two = scale * second_weight / size_norm * factor
        factor_one = scale * first_weight / size_norm * inverse - factor_two * along
        for at, c_ref in ((0, ca_ref), (rows, cb_ref)):
            span = slice(at, at + rows)
            outs[0][span, :] = factor_one * vector_ref[span, :] + factor_two * c_ref[:rows, :]
            outs[1][span, :] = factor_one * image_ref[span, :] + factor_two * second_ref[span, :]
        row = lax.broadcasted_iota(jnp.int32, (EDGE, m), 1)
        outs[2][...] = jnp.where(row == 0, theta, lowest)

    state, image, energies = kernel_call(
        finish, [array(2 * rows, m), array(2 * rows, m), array(EDGE, m)], [second],
        [vector, image_own, own_c[0], own_c[1]], [sums],
    )
    return (state[None], image[None], energies[0, :2])


def solution(mesh):
    in_specs = (
        P("sector", "pair", None),
        P("sector", "pair", None),
        P("pair", "sector", None, None),
        P("pair", "sector", None, None),
        P("pair"),
        P("sector", None),
    )
    out_specs = (P("sector", "pair", None), P("sector", "pair", None), P())
    return jax.shard_map(
        per_device, mesh=mesh, in_specs=in_specs, out_specs=out_specs, check_vma=False
    )
```

```python
import math

import jax
import jax.numpy as jnp
from jax import lax
from jax.experimental import pallas as pl
from jax.experimental.pallas import tpu as pltpu
from jax.sharding import PartitionSpec as P


F32, BF16 = jnp.float32, jnp.bfloat16
LIMIT = 12 * 1024 * 1024
X, Y = 1, 2
EDGE = 8


def deep_masks(count):
    bits = [4 << b for b in range((count // 4).bit_length() - 1)]
    return bits[:1] + [bits[0] | bits[1]] + bits[2:] if len(bits) > 1 else bits


def streams(count):
    deep = deep_masks(count)
    return deep + [X, Y], deep + [Y, X]


def offsets(masks):
    slots = [0]
    for mask in masks:
        slots = slots + [slot ^ mask for slot in slots]
    return slots


def row_order(count):
    a, b = (offsets(masks) for masks in streams(count))
    middle = count // 2
    return (
        [(s, 0) for s in a[:middle]] + [(s, 1) for s in b[:middle]]
        + [(s, 0) for s in a[middle:]] + [(s, 1) for s in b[middle:]]
    )


def swap(block, mask):
    return lax.ppermute(block, "pair", [(i, i ^ mask) for i in range(lax.axis_size("pair"))])


def shifted(block, distance):
    size = lax.axis_size("sector")
    return lax.ppermute(block, "sector", [((i - distance) % size, i) for i in range(size)])


def neighbours(block):
    if lax.axis_size("sector") == 2:
        return [shifted(block, 1)]
    return [shifted(block, 1), shifted(block, -1)]


def to_neighbours(blocks):
    if lax.axis_size("sector") == 2:
        return [shifted(blocks[0], 1)]
    return [shifted(blocks[0], -1), shifted(blocks[1], 1)]


def over_sectors(tile):
    if lax.axis_size("sector") == 2:
        return [tile, shifted(tile, 1)]
    return [lax.psum(tile, "sector")]


def array(*shape, kind=F32):
    return jax.ShapeDtypeStruct(shape, kind)


def kernel_call(body, outs, *groups, scratch=(), flops=0, scalar_outs=0):
    flat = [value for group in groups for value in group]

    def kernel(*refs):
        refs = list(refs)
        take = lambda n: [refs.pop(0) for _ in range(n)]
        inputs = [take(len(group)) for group in groups]
        body(inputs, take(len(outs)), refs)

    traffic = sum(v.size * v.dtype.itemsize for v in flat)
    return pl.pallas_call(
        kernel,
        in_specs=[pl.BlockSpec(memory_space=pltpu.VMEM)] * len(flat),
        out_specs=[pl.BlockSpec(memory_space=pltpu.VMEM)] * (len(outs) - scalar_outs)
        + [pl.BlockSpec(memory_space=pltpu.SMEM)] * scalar_outs,
        out_shape=list(outs),
        scratch_shapes=list(scratch),
        compiler_params=pltpu.CompilerParams(vmem_limit_bytes=LIMIT),
        cost_estimate=pl.CostEstimate(flops=max(flops, traffic), bytes_accessed=traffic, transcendentals=0),
    )(*flat)


def split(value):
    high = value.astype(BF16)
    return high, (value - high.astype(F32)).astype(BF16)


def dot(first, second):
    return jnp.dot(first, second, preferred_element_type=F32)


def dot3(first, second):
    return dot(first[0], second[0]) + dot(first[0], second[1]) + dot(first[1], second[0])


def tile_rows(values):
    shape = (EDGE, values[0].shape[1])
    row = lax.broadcasted_iota(jnp.int32, shape, 0)
    tile = jnp.zeros(shape, F32)
    for at, value in enumerate(values):
        tile = jnp.where(row == at, value, tile)
    return tile


def summed(value, width):
    return jnp.broadcast_to(jnp.sum(value, keepdims=True), (1, width))


def block_of(charge, sectors):
    return jnp.where(charge == 1, 0, 1 if sectors == 2 else jnp.where(charge == 0, 1, 2))


def prepare(me, charges, coupling, left_ops, right_ops, block, count):
    pairs, _, m, _ = left_ops.shape
    rows = m // count // 2
    order = row_order(count)
    sectors = lax.axis_size("sector")

    def kernel(me_ref, charges_ref, coupling_ref, left_ref, right_ref, block_ref, *refs):
        left_out, left_t_out, right_out, right_t_out, edge, table, held = refs

        def reorder(value):
            held[...] = value
            parts = []
            for slot, half in order:
                where = pl.multiple_of((me_ref[0] ^ slot) * (2 * rows) + half * rows, rows)
                parts.append(held[pl.ds(where, rows), :])
            return jnp.concatenate(parts, axis=0)

        turned = reorder(reorder(left_ref[...]).T)
        left_t_out[0], left_t_out[1] = split(turned)
        left_out[0], left_out[1] = split(turned.T)
        value = right_ref[...]
        right_out[0], right_out[1] = split(value)
        right_t_out[0], right_t_out[1] = split(value.T)
        edge[...] = tile_rows([jnp.zeros((1, m), F32), summed(block_ref[...] * block_ref[...], m)])
        row = lax.broadcasted_iota(jnp.int32, table.shape, 0)
        values = jnp.zeros(table.shape, jnp.int32)
        for pair in range(pairs):
            charge = charges_ref[pair]
            values = jnp.where(row == 2 * pair, block_of(charge, sectors), values)
            values = jnp.where(row == 2 * pair + 1, coupling_ref[0, charge], values)
        table[...] = values

    source = pl.BlockSpec((None, None, m, m), lambda p, *_: (p, 0, 0, 0))
    target = pl.BlockSpec((None, 2, m, m), lambda p, *_: (p, 0, 0, 0))
    whole = pl.BlockSpec(memory_space=pltpu.VMEM)
    return pl.pallas_call(
        kernel,
        grid_spec=pltpu.PrefetchScalarGridSpec(
            num_scalar_prefetch=3,
            grid=(pairs,),
            in_specs=[source, source, whole],
            out_specs=[target] * 4 + [whole] * 2,
            scratch_shapes=[pltpu.VMEM((m, m), F32)],
        ),
        out_shape=[array(pairs, 2, m, m, kind=BF16)] * 4
        + [array(EDGE, m), array(-(-2 * pairs // 8) * 8, 128, kind=jnp.int32)],
        compiler_params=pltpu.CompilerParams(vmem_limit_bytes=10 * LIMIT // 3),
        cost_estimate=pl.CostEstimate(flops=pairs * m * m * 1500, bytes_accessed=24 * pairs * m * m, transcendentals=0),
    )(me, charges, coupling, left_ops, right_ops, block)


def double(block, masks):
    for mask in masks:
        more = swap(block, mask)
        rows, m = block.shape[0] // 2, block.shape[1]

        def meet_column(inputs, outs, scratch):
            (low, high), (out,) = inputs[0], outs
            for part in (0, 1):
                span = slice(part * rows, (part + 1) * rows)
                out[2 * part * rows : (2 * part + 1) * rows, :] = low[span, :]
                out[(2 * part + 1) * rows : (2 * part + 2) * rows, :] = high[span, :]

        (block,) = kernel_call(meet_column, [array(4 * rows, m)], [block, more])
    return block


def sigma_apply(column_a, column_b, ops, table, edge):
    left, left_t, right, right_t = ops
    pairs, m = left.shape[0], left.shape[2]
    sectors = lax.axis_size("sector")
    blocks = min(sectors, 3)
    half, quarter, eighth = m // 2, m // 4, m // 8
    rows_of = array(half, m)
    made = array(pairs, 2, half, m, kind=BF16)
    held = pltpu.VMEM((blocks, 2, half, m), BF16)
    cost = 6 * half * m * m * pairs

    def hold(scratch, groups):
        for block, group in enumerate(groups):
            at = 0
            for ref in group:
                size = ref.shape[0]
                scratch[block, 0, at : at + size, :], scratch[block, 1, at : at + size, :] = split(ref[...])
                at += size

    def gains(fixed, pair):
        block = jnp.max(fixed[2 * pair : 2 * pair + 1, :])
        return block, fixed[2 * pair + 1 : 2 * pair + 2, :1].astype(F32)

    def parts(ref, *index):
        return ref[index[0], 0], ref[index[0], 1]

    more_a, more_b = swap(column_a, X), swap(column_b, Y)

    def join(inputs, outs, scratch):
        both, a, b = outs
        for at, (low, high), out in ((0, inputs[0], a), (quarter, inputs[1], b)):
            out[:eighth, :] = low[...]
            out[eighth:, :] = high[...]
            both[at : at + eighth, :] = low[...]
            both[at + eighth : at + quarter, :] = high[...]

    early, a, b = kernel_call(
        join, [rows_of, array(quarter, m), array(quarter, m)], [column_a, more_a], [column_b, more_b]
    )
    early_others = neighbours(early)
    late = [swap(a, Y), swap(b, X)]

    def outer(ref, pair, at, start, inner):
        rows, columns = slice(at, at + half), slice(start, start + half)
        return dot3((ref[pair, 0, rows, columns], ref[pair, 1, rows, columns]), inner)

    def first_inner(inputs, outs, scratch):
        (own, *others), (rights,), (rights_t,), (lefts,), (lefts_t,), (fixed,) = inputs
        z_out, y_out, back_out = outs[:3]
        held_ref, total = scratch
        hold(held_ref, [[own]] + [[other] for other in others])
        total[...] = jnp.zeros_like(total)
        back = jnp.zeros((half, m), F32)
        for pair in range(pairs):
            block, allowed = gains(fixed, pair)
            forward = split(dot3(parts(held_ref, 0), parts(rights_t, pair)) * allowed)
            z_out[pair, 0], z_out[pair, 1] = forward
            total[block] = total[block] + outer(lefts, pair, half, 0, forward)
            backward = split(dot3((held_ref[block, 0], held_ref[block, 1]), parts(rights, pair)) * allowed)
            y_out[pair, 0], y_out[pair, 1] = backward
            back = back + outer(lefts_t, pair, half, 0, backward)
        back_out[...] = back
        for block in range(blocks):
            outs[3 + block][...] = total[block]

    totals = pltpu.VMEM((blocks, half, m), F32)
    early_z, early_y, early_back, *early_terms = kernel_call(
        first_inner, [made] * 2 + [rows_of] * (1 + blocks), [early] + early_others, [right], [right_t], [left],
        [left_t], [table], scratch=[held, totals], flops=3 * cost,
    )
    late_others = [neighbours(piece) for piece in late]
    late_others = [[late_others[q][b] for q in range(2)] for b in range(blocks - 1)]

    def forward_late(inputs, outs, scratch):
        own, terms, (rights_t,), (lefts,), (fixed,) = inputs
        z_out, (held_ref, total) = outs[0], scratch
        hold(held_ref, [own])
        for block in range(blocks):
            total[block] = terms[block][...]
        for pair in range(pairs):
            block, allowed = gains(fixed, pair)
            inner = split(dot3(parts(held_ref, 0), parts(rights_t, pair)) * allowed)
            z_out[pair, 0], z_out[pair, 1] = inner
            total[block] = total[block] + outer(lefts, pair, half, half, inner)
        for block in range(blocks):
            outs[1 + block][...] = total[block]

    late_z, own_sent, *aimed = kernel_call(
        forward_late, [made] + [rows_of] * blocks, late, early_terms, [right_t], [left], [table],
        scratch=[held, totals], flops=2 * cost,
    )
    aimed_sent = to_neighbours(aimed)

    def backward_late(inputs, outs, scratch):
        groups, (rights,), (lefts_t,), (base, back_ref), (fixed,) = inputs
        y_out, sent, product = outs
        hold(scratch[0], [groups[2 * block : 2 * block + 2] for block in range(blocks)])
        total = back_ref[...]
        for pair in range(pairs):
            block, allowed = gains(fixed, pair)
            inner = split(dot3((scratch[0][block, 0], scratch[0][block, 1]), parts(rights, pair)) * allowed)
            y_out[pair, 0], y_out[pair, 1] = inner
            total = total + outer(lefts_t, pair, half, half, inner)
        sent[...] = total + base[...]
        own = jnp.concatenate([groups[0][...], groups[1][...]], axis=0)
        product[...] = jnp.broadcast_to(summed(own * total, m), (EDGE, m))

    late_y, own_sent, product = kernel_call(
        backward_late, [made, rows_of, array(EDGE, m)], late + sum(late_others, []), [right], [left_t],
        [own_sent, early_back], [table], scratch=[held], flops=2 * cost,
    )

    def add_sent(inputs, outs, scratch):
        value = sum(ref[...] for ref in inputs[0])
        outs[0][...] = value[:quarter]
        outs[1][...] = value[quarter:]

    sent_a, sent_b = kernel_call(add_sent, [array(quarter, m)] * 2, [own_sent] + aimed_sent)
    got_a, got_b = swap(sent_a, Y), swap(sent_b, X)

    def keep(inputs, outs, scratch):
        (z0, z1), (y0, y1), (lefts,), (lefts_t,), (own, product_ref, edge_ref), (fixed,) = inputs
        total = scratch[0]
        total[...] = jnp.zeros_like(total)
        back = jnp.zeros((half, m), F32)
        for pair in range(pairs):
            block, _ = gains(fixed, pair)
            term = outer(lefts, pair, 0, 0, parts(z0, pair)) + outer(lefts, pair, 0, half, parts(z1, pair))
            total[block] = total[block] + term
        for block in range(1, blocks):
            outs[1 + block][...] = total[block]
        for pair in range(pairs):
            back = back + outer(lefts_t, pair, 0, 0, parts(y0, pair))
            back = back + outer(lefts_t, pair, 0, half, parts(y1, pair))
        outs[0][...] = total[0] + back
        product_sum = 2.0 * (summed(own[...] * back, m) + product_ref[:1, :])
        row = lax.broadcasted_iota(jnp.int32, (EDGE, m), 0)
        outs[1][...] = jnp.where(row == 0, product_sum, edge_ref[...])

    own_kept, edge, *aimed = kernel_call(
        keep, [rows_of, array(EDGE, m)] + [rows_of] * (blocks - 1), [early_z, late_z], [early_y, late_y], [left],
        [left_t], [early, product, edge], [table],
        scratch=[totals], flops=2 * cost,
    )
    aimed_kept = to_neighbours(aimed)
    edges = over_sectors(edge)

    def first_sum(inputs, outs, scratch):
        kept, (a_ref, b_ref), edge_refs = inputs
        value = sum(ref[...] for ref in kept)
        edge_sum = sum(ref[...] for ref in edge_refs)
        a_value, b_value = value[:quarter] + a_ref[...], value[quarter:] + b_ref[...]
        for (stay, go), total in ((outs[:2], a_value), (outs[2:4], b_value)):
            stay[...] = total[:eighth]
            go[:eighth, :] = total[eighth:]
            go[eighth:, :] = edge_sum
        outs[4][...] = edge_sum

    stay_a, go_a, stay_b, go_b, edge = kernel_call(
        first_sum, [array(eighth, m), array(eighth + EDGE, m)] * 2 + [array(EDGE, m)],
        [own_kept] + aimed_kept, [got_a, got_b], edges,
    )
    got_a, got_b, corner = swap(go_a, X), swap(go_b, Y), swap(edge, X | Y)

    def second_sum(inputs, outs, scratch):
        (a_stay, a_got), (b_stay, b_got), (edge_ref, corner_ref) = inputs
        outs[0][:eighth, :] = a_stay[...] + a_got[:eighth, :]
        outs[0][eighth:quarter, :] = b_stay[...] + b_got[:eighth, :]
        outs[0][quarter:, :] = edge_ref[...] + a_got[eighth:, :] + b_got[eighth:, :] + corner_ref[...]

    return kernel_call(second_sum, [array(quarter + EDGE, m)], [stay_a, got_a], [stay_b, got_b], [edge, corner])[0]


def turned(value, slots, mask, rows):
    size = len(slots) * rows
    parts = [
        value[part * size + slots.index(slot ^ mask) * rows :][:rows] for part in (0, 1) for slot in slots
    ]
    return jnp.concatenate(parts + [value[2 * size :]], axis=0)


def per_device(wavefunction, preconditioner, left_ops, right_ops, charges, coupling):
    vector, divisor = wavefunction[0], preconditioner[0]
    count = lax.axis_size("pair")
    deep = deep_masks(count)
    slots = offsets(deep)
    rows, m = vector.shape[0] // 2, vector.shape[1]
    tall = rows * len(slots)
    me = lax.axis_index("pair").astype(jnp.int32)[None]

    def load(inputs, outs, scratch):
        outs[0][...] = inputs[0][0][...]

    (vector,) = kernel_call(load, [array(2 * rows, m)], [vector])
    *ops, edge, table = prepare(me, charges, coupling, left_ops, right_ops, vector, count)
    column = double(vector, deep)
    divisor = double(divisor, deep)

    def part(inputs, outs, scratch):
        outs[0][...] = inputs[0][0][:tall, :]
        outs[1][...] = inputs[0][0][tall:, :]

    vector_a, vector_b = kernel_call(part, [array(tall, m)] * 2, [column])
    image = sigma_apply(vector_a, vector_b, ops, table, edge)
    for mask in deep[:0:-1]:

        def add_columns(inputs, outs, scratch):
            own, got = inputs[0]
            outs[0][...] = own[...] + turned(got[...], slots, mask, rows)

        (image,) = kernel_call(add_columns, [array(*image.shape)], [image, swap(image, mask)])

    def correct(inputs, outs, scratch):
        own, got, w_ref, p_ref = inputs[0]
        correction_a, correction_b, image_own, sums_out, edge_out = outs
        total = own[...] + turned(got[...], slots, deep[0], rows)
        sums = total[2 * tall :]
        theta = sums[0:1, :] / sums[1:2, :]
        c = (total[: 2 * tall] - theta * w_ref[...]) / p_ref[...]
        correction_a[...] = c[:tall]
        correction_b[...] = c[tall:]
        sums_out[...] = sums

        def owned(value):
            return jnp.concatenate([value[:rows], value[tall : tall + rows]], axis=0)

        own_w, own_c, own_a = owned(w_ref[...]), owned(c), owned(total)
        image_own[...] = own_a
        edge_out[...] = tile_rows(
            [jnp.zeros((1, m), F32), summed(own_w * own_c, m), summed(own_c * own_c, m), summed(own_a * own_c, m)]
        )

    ca, cb, image_own, sums, edge = kernel_call(
        correct, [array(tall, m), array(tall, m), array(2 * rows, m), array(EDGE, m), array(EDGE, m)],
        [image, swap(image, deep[0]), column, divisor],
    )
    own_c = (ca, cb)
    second = sigma_apply(ca, cb, ops, table, edge)

    for mask in deep[::-1]:
        size = (second.shape[0] - EDGE) // 4

        def cut(inputs, outs, scratch):
            ref, out = inputs[0][0], outs[0]
            out[:size, :] = ref[size : 2 * size, :]
            out[size:, :] = ref[3 * size :, :]

        def meet(inputs, outs, scratch):
            (ref, got), out = inputs[0], outs[0]
            out[:size, :] = ref[:size, :] + got[:size, :]
            out[size : 2 * size, :] = ref[2 * size : 3 * size, :] + got[size : 2 * size, :]
            out[2 * size :, :] = ref[4 * size :, :] + got[2 * size :, :]

        shape = [array(2 * size + EDGE, m)]
        (go,) = kernel_call(cut, shape, [second])
        (second,) = kernel_call(meet, shape, [second, swap(go, mask)])

    scale = math.sqrt(lax.axis_size("sector") * count * vector.shape[0] * m)

    def finish(inputs, outs, scratch):
        (second_ref,), (vector_ref, image_ref, ca_ref, cb_ref), (first_ref,) = inputs
        sums = second_ref[2 * rows :, :]
        correlation, norm_sq = first_ref[0:1, :], first_ref[1:2, :]
        theta = correlation / norm_sq
        inverse = lax.rsqrt(norm_sq)
        along = sums[1:2] / norm_sq
        length_sq = (sums[2:3] - along * sums[1:2]) / norm_sq
        factor = inverse * lax.rsqrt(length_sq + 1e-30)
        corner = factor * factor * (sums[0:1] - 2.0 * along * sums[3:4] + along * along * correlation)
        cross = inverse * factor * (sums[3:4] - along * correlation)
        spread = (theta - corner) / 2.0
        lowest = (theta + corner) / 2.0 - jnp.sqrt(spread * spread + cross * cross)
        first_weight = corner - lowest
        second_weight = -cross
        size_norm = jnp.sqrt(first_weight * first_weight + second_weight * second_weight + 1e-30)
        factor_two = scale * second_weight / size_norm * factor
        factor_one = scale * first_weight / size_norm * inverse - factor_two * along
        for at, c_ref in ((0, ca_ref), (rows, cb_ref)):
            span = slice(at, at + rows)
            outs[0][span, :] = factor_one * vector_ref[span, :] + factor_two * c_ref[:rows, :]
            outs[1][span, :] = factor_one * image_ref[span, :] + factor_two * second_ref[span, :]
        outs[2][0] = jnp.max(theta)
        outs[2][1] = jnp.max(lowest)

    state, image, energies = kernel_call(
        finish, [array(2 * rows, m), array(2 * rows, m), array(2)], [second],
        [vector, image_own, own_c[0], own_c[1]], [sums], scalar_outs=1,
    )
    return (state[None], image[None], energies)


def solution(mesh):
    in_specs = (
        P("sector", "pair", None),
        P("sector", "pair", None),
        P("pair", "sector", None, None),
        P("pair", "sector", None, None),
        P("pair"),
        P("sector", None),
    )
    out_specs = (P("sector", "pair", None), P("sector", "pair", None), P())
    return jax.shard_map(
        per_device, mesh=mesh, in_specs=in_specs, out_specs=out_specs, check_vma=False
    )
```

```python
import math

import jax
import jax.numpy as jnp
from jax import lax
from jax.experimental import pallas as pl
from jax.experimental.pallas import tpu as pltpu
from jax.sharding import PartitionSpec as P


F32, BF16 = jnp.float32, jnp.bfloat16
LIMIT = 12 * 1024 * 1024
PREPARE_LIMIT = 40 * 1024 * 1024
X, Y = 1, 2
EDGE = 8


def deep_masks(count):
    bits = [4 << b for b in range((count // 4).bit_length() - 1)]
    return bits[:1] + [bits[0] | bits[1]] + bits[2:] if len(bits) > 1 else bits


def streams(count):
    deep = deep_masks(count)
    return deep + [X, Y], deep + [Y, X]


def offsets(masks):
    slots = [0]
    for mask in masks:
        slots = slots + [slot ^ mask for slot in slots]
    return slots


def row_order(count):
    a, b = (offsets(masks) for masks in streams(count))
    middle = count // 2
    return (
        [(s, 0) for s in a[:middle]] + [(s, 1) for s in b[:middle]]
        + [(s, 0) for s in a[middle:]] + [(s, 1) for s in b[middle:]]
    )


def swap(block, mask):
    return lax.ppermute(block, "pair", [(i, i ^ mask) for i in range(lax.axis_size("pair"))])


def shifted(block, distance):
    size = lax.axis_size("sector")
    return lax.ppermute(block, "sector", [((i - distance) % size, i) for i in range(size)])


def neighbours(block):
    if lax.axis_size("sector") == 2:
        return [shifted(block, 1)]
    return [shifted(block, 1), shifted(block, -1)]


def to_neighbours(blocks):
    if lax.axis_size("sector") == 2:
        return [shifted(blocks[0], 1)]
    return [shifted(blocks[0], -1), shifted(blocks[1], 1)]


def over_sectors(tile):
    if lax.axis_size("sector") == 2:
        return [tile, shifted(tile, 1)]
    return [lax.psum(tile, "sector")]


def array(*shape, kind=F32):
    return jax.ShapeDtypeStruct(shape, kind)


def kernel_call(body, outs, *groups, scratch=(), flops=0, scalar_outs=0):
    flat = [value for group in groups for value in group]

    def kernel(*refs):
        refs = list(refs)
        take = lambda n: [refs.pop(0) for _ in range(n)]
        inputs = [take(len(group)) for group in groups]
        body(inputs, take(len(outs)), refs)

    traffic = sum(v.size * v.dtype.itemsize for v in flat)
    return pl.pallas_call(
        kernel,
        in_specs=[pl.BlockSpec(memory_space=pltpu.VMEM)] * len(flat),
        out_specs=[pl.BlockSpec(memory_space=pltpu.VMEM)] * (len(outs) - scalar_outs)
        + [pl.BlockSpec(memory_space=pltpu.SMEM)] * scalar_outs,
        out_shape=list(outs),
        scratch_shapes=list(scratch),
        compiler_params=pltpu.CompilerParams(vmem_limit_bytes=LIMIT),
        cost_estimate=pl.CostEstimate(flops=max(flops, traffic), bytes_accessed=traffic, transcendentals=0),
    )(*flat)


def split(value):
    high = value.astype(BF16)
    return high, (value - high.astype(F32)).astype(BF16)


def dot(first, second):
    return jnp.dot(first, second, preferred_element_type=F32)


def dot3(first, second):
    return dot(first[0], second[0]) + dot(first[0], second[1]) + dot(first[1], second[0])


def tile_rows(values):
    shape = (EDGE, values[0].shape[1])
    row = lax.broadcasted_iota(jnp.int32, shape, 0)
    tile = jnp.zeros(shape, F32)
    for at, value in enumerate(values):
        tile = jnp.where(row == at, value, tile)
    return tile


def summed(value, width):
    return jnp.broadcast_to(jnp.sum(value, keepdims=True), (1, width))


def block_of(charge, sectors):
    return jnp.where(charge == 1, 0, 1 if sectors == 2 else jnp.where(charge == 0, 1, 2))


def tabulate(charges, coupling):
    pairs, sectors = charges.shape[0], lax.axis_size("sector")

    def kernel(charges_ref, coupling_ref, table):
        row = lax.broadcasted_iota(jnp.int32, table.shape, 0)
        values = jnp.zeros(table.shape, jnp.int32)
        for pair in range(pairs):
            charge = charges_ref[pair]
            values = jnp.where(row == 2 * pair, block_of(charge, sectors), values)
            values = jnp.where(row == 2 * pair + 1, coupling_ref[0, charge], values)
        table[...] = values

    return pl.pallas_call(
        kernel,
        in_specs=[pl.BlockSpec(memory_space=pltpu.SMEM)] * 2,
        out_specs=pl.BlockSpec(memory_space=pltpu.VMEM),
        out_shape=array(-(-2 * pairs // 8) * 8, 128, kind=jnp.int32),
        compiler_params=pltpu.CompilerParams(vmem_limit_bytes=LIMIT),
        cost_estimate=pl.CostEstimate(flops=10**6, bytes_accessed=4096, transcendentals=0),
    )(charges, coupling)


def prepare(me, left_ops, right_ops, block, count):
    pairs, _, m, _ = left_ops.shape
    rows = m // count // 2
    order = row_order(count)

    def kernel(me_ref, left_ref, right_ref, block_ref, *refs):
        left_out, left_t_out, right_out, right_t_out, edge, held = refs

        def reorder(value):
            held[...] = value
            parts = []
            for slot, half in order:
                where = pl.multiple_of((me_ref[0] ^ slot) * (2 * rows) + half * rows, rows)
                parts.append(held[pl.ds(where, rows), :])
            return jnp.concatenate(parts, axis=0)

        turned = reorder(reorder(left_ref[...]).T)
        left_t_out[0], left_t_out[1] = split(turned)
        left_out[0], left_out[1] = split(turned.T)
        value = right_ref[...]
        right_out[0], right_out[1] = split(value)
        right_t_out[0], right_t_out[1] = split(value.T)
        edge[...] = tile_rows([jnp.zeros((1, m), F32), summed(block_ref[...] * block_ref[...], m)])

    source = pl.BlockSpec((None, None, m, m), lambda p, *_: (p, 0, 0, 0))
    target = pl.BlockSpec((None, 2, m, m), lambda p, *_: (p, 0, 0, 0))
    whole = pl.BlockSpec(memory_space=pltpu.VMEM)
    return pl.pallas_call(
        kernel,
        grid_spec=pltpu.PrefetchScalarGridSpec(
            num_scalar_prefetch=1,
            grid=(pairs,),
            in_specs=[source, source, whole],
            out_specs=[target] * 4 + [whole],
            scratch_shapes=[pltpu.VMEM((m, m), F32)],
        ),
        out_shape=[array(pairs, 2, m, m, kind=BF16)] * 4 + [array(EDGE, m)],
        compiler_params=pltpu.CompilerParams(vmem_limit_bytes=PREPARE_LIMIT),
        cost_estimate=pl.CostEstimate(flops=pairs * m * m * 1500, bytes_accessed=24 * pairs * m * m, transcendentals=0),
    )(me, left_ops, right_ops, block)


def double(block, masks):
    for mask in masks:
        more = swap(block, mask)
        rows, m = block.shape[0] // 2, block.shape[1]

        def meet_column(inputs, outs, scratch):
            (low, high), (out,) = inputs[0], outs
            for part in (0, 1):
                span = slice(part * rows, (part + 1) * rows)
                out[2 * part * rows : (2 * part + 1) * rows, :] = low[span, :]
                out[(2 * part + 1) * rows : (2 * part + 2) * rows, :] = high[span, :]

        (block,) = kernel_call(meet_column, [array(4 * rows, m)], [block, more])
    return block


def sigma_apply(column_a, column_b, ops, table, edge):
    left, left_t, right, right_t = ops
    pairs, m = left.shape[0], left.shape[2]
    sectors = lax.axis_size("sector")
    blocks = min(sectors, 3)
    half, quarter, eighth = m // 2, m // 4, m // 8
    rows_of = array(half, m)
    made = array(pairs, 2, half, m, kind=BF16)
    held = pltpu.VMEM((blocks, 2, half, m), BF16)
    cost = 6 * half * m * m * pairs

    def hold(scratch, groups):
        for block, group in enumerate(groups):
            at = 0
            for ref in group:
                size = ref.shape[0]
                scratch[block, 0, at : at + size, :], scratch[block, 1, at : at + size, :] = split(ref[...])
                at += size

    def gains(fixed, pair):
        block = jnp.max(fixed[2 * pair : 2 * pair + 1, :])
        return block, fixed[2 * pair + 1 : 2 * pair + 2, :1].astype(F32)

    def parts(ref, *index):
        return ref[index[0], 0], ref[index[0], 1]

    more_a, more_b = swap(column_a, X), swap(column_b, Y)

    def join(inputs, outs, scratch):
        both, a, b = outs
        for at, (low, high), out in ((0, inputs[0], a), (quarter, inputs[1], b)):
            out[:eighth, :] = low[...]
            out[eighth:, :] = high[...]
            both[at : at + eighth, :] = low[...]
            both[at + eighth : at + quarter, :] = high[...]

    early, a, b = kernel_call(
        join, [rows_of, array(quarter, m), array(quarter, m)], [column_a, more_a], [column_b, more_b]
    )
    early_others = neighbours(early)
    late = [swap(a, Y), swap(b, X)]

    def outer(ref, pair, at, start, inner):
        rows, columns = slice(at, at + half), slice(start, start + half)
        return dot3((ref[pair, 0, rows, columns], ref[pair, 1, rows, columns]), inner)

    def first_inner(inputs, outs, scratch):
        (own, *others), (rights,), (rights_t,), (lefts,), (lefts_t,), (fixed,) = inputs
        z_out, y_out, back_out = outs[:3]
        held_ref, total = scratch
        hold(held_ref, [[own]] + [[other] for other in others])
        total[...] = jnp.zeros_like(total)
        back = jnp.zeros((half, m), F32)
        for pair in range(pairs):
            block, allowed = gains(fixed, pair)
            forward = split(dot3(parts(held_ref, 0), parts(rights_t, pair)) * allowed)
            z_out[pair, 0], z_out[pair, 1] = forward
            total[block] = total[block] + outer(lefts, pair, half, 0, forward)
            backward = split(dot3((held_ref[block, 0], held_ref[block, 1]), parts(rights, pair)) * allowed)
            y_out[pair, 0], y_out[pair, 1] = backward
            back = back + outer(lefts_t, pair, half, 0, backward)
        back_out[...] = back
        for block in range(blocks):
            outs[3 + block][...] = total[block]

    totals = pltpu.VMEM((blocks, half, m), F32)
    early_z, early_y, early_back, *early_terms = kernel_call(
        first_inner, [made] * 2 + [rows_of] * (1 + blocks), [early] + early_others, [right], [right_t], [left],
        [left_t], [table], scratch=[held, totals], flops=3 * cost,
    )
    late_others = [neighbours(piece) for piece in late]
    late_others = [[late_others[q][b] for q in range(2)] for b in range(blocks - 1)]

    def forward_late(inputs, outs, scratch):
        own, terms, (rights_t,), (lefts,), (fixed,) = inputs
        z_out, (held_ref, total) = outs[0], scratch
        hold(held_ref, [own])
        for block in range(blocks):
            total[block] = terms[block][...]
        for pair in range(pairs):
            block, allowed = gains(fixed, pair)
            inner = split(dot3(parts(held_ref, 0), parts(rights_t, pair)) * allowed)
            z_out[pair, 0], z_out[pair, 1] = inner
            total[block] = total[block] + outer(lefts, pair, half, half, inner)
        for block in range(blocks):
            outs[1 + block][...] = total[block]

    late_z, own_sent, *aimed = kernel_call(
        forward_late, [made] + [rows_of] * blocks, late, early_terms, [right_t], [left], [table],
        scratch=[held, totals], flops=2 * cost,
    )
    aimed_sent = to_neighbours(aimed)

    def backward_late(inputs, outs, scratch):
        groups, (rights,), (lefts_t,), (base, back_ref), (fixed,) = inputs
        y_out, sent, product = outs
        hold(scratch[0], [groups[2 * block : 2 * block + 2] for block in range(blocks)])
        total = back_ref[...]
        for pair in range(pairs):
            block, allowed = gains(fixed, pair)
            inner = split(dot3((scratch[0][block, 0], scratch[0][block, 1]), parts(rights, pair)) * allowed)
            y_out[pair, 0], y_out[pair, 1] = inner
            total = total + outer(lefts_t, pair, half, half, inner)
        sent[...] = total + base[...]
        own = jnp.concatenate([groups[0][...], groups[1][...]], axis=0)
        product[...] = jnp.broadcast_to(summed(own * total, m), (EDGE, m))

    late_y, own_sent, product = kernel_call(
        backward_late, [made, rows_of, array(EDGE, m)], late + sum(late_others, []), [right], [left_t],
        [own_sent, early_back], [table], scratch=[held], flops=2 * cost,
    )

    def add_sent(inputs, outs, scratch):
        value = sum(ref[...] for ref in inputs[0])
        outs[0][...] = value[:quarter]
        outs[1][...] = value[quarter:]

    sent_a, sent_b = kernel_call(add_sent, [array(quarter, m)] * 2, [own_sent] + aimed_sent)
    got_a, got_b = swap(sent_a, Y), swap(sent_b, X)

    def keep(inputs, outs, scratch):
        (z0, z1), (y0, y1), (lefts,), (lefts_t,), (own, product_ref, edge_ref), (fixed,) = inputs
        total = scratch[0]
        total[...] = jnp.zeros_like(total)
        back = jnp.zeros((half, m), F32)
        for pair in range(pairs):
            block, _ = gains(fixed, pair)
            term = outer(lefts, pair, 0, 0, parts(z0, pair)) + outer(lefts, pair, 0, half, parts(z1, pair))
            total[block] = total[block] + term
        for block in range(1, blocks):
            outs[1 + block][...] = total[block]
        for pair in range(pairs):
            back = back + outer(lefts_t, pair, 0, 0, parts(y0, pair))
            back = back + outer(lefts_t, pair, 0, half, parts(y1, pair))
        outs[0][...] = total[0] + back
        product_sum = 2.0 * (summed(own[...] * back, m) + product_ref[:1, :])
        row = lax.broadcasted_iota(jnp.int32, (EDGE, m), 0)
        outs[1][...] = jnp.where(row == 0, product_sum, edge_ref[...])

    own_kept, edge, *aimed = kernel_call(
        keep, [rows_of, array(EDGE, m)] + [rows_of] * (blocks - 1), [early_z, late_z], [early_y, late_y], [left],
        [left_t], [early, product, edge], [table],
        scratch=[totals], flops=2 * cost,
    )
    aimed_kept = to_neighbours(aimed)
    edges = over_sectors(edge)

    def first_sum(inputs, outs, scratch):
        kept, (a_ref, b_ref), edge_refs = inputs
        value = sum(ref[...] for ref in kept)
        edge_sum = sum(ref[...] for ref in edge_refs)
        a_value, b_value = value[:quarter] + a_ref[...], value[quarter:] + b_ref[...]
        for (stay, go), total in ((outs[:2], a_value), (outs[2:4], b_value)):
            stay[...] = total[:eighth]
            go[:eighth, :] = total[eighth:]
            go[eighth:, :] = edge_sum
        outs[4][...] = edge_sum

    stay_a, go_a, stay_b, go_b, edge = kernel_call(
        first_sum, [array(eighth, m), array(eighth + EDGE, m)] * 2 + [array(EDGE, m)],
        [own_kept] + aimed_kept, [got_a, got_b], edges,
    )
    got_a, got_b, corner = swap(go_a, X), swap(go_b, Y), swap(edge, X | Y)

    def second_sum(inputs, outs, scratch):
        (a_stay, a_got), (b_stay, b_got), (edge_ref, corner_ref) = inputs
        outs[0][:eighth, :] = a_stay[...] + a_got[:eighth, :]
        outs[0][eighth:quarter, :] = b_stay[...] + b_got[:eighth, :]
        outs[0][quarter:, :] = edge_ref[...] + a_got[eighth:, :] + b_got[eighth:, :] + corner_ref[...]

    return kernel_call(second_sum, [array(quarter + EDGE, m)], [stay_a, got_a], [stay_b, got_b], [edge, corner])[0]


def turned(value, slots, mask, rows):
    size = len(slots) * rows
    parts = [
        value[part * size + slots.index(slot ^ mask) * rows :][:rows] for part in (0, 1) for slot in slots
    ]
    return jnp.concatenate(parts + [value[2 * size :]], axis=0)


def per_device(wavefunction, preconditioner, left_ops, right_ops, charges, coupling):
    vector, divisor = wavefunction[0], preconditioner[0]
    count = lax.axis_size("pair")
    deep = deep_masks(count)
    slots = offsets(deep)
    rows, m = vector.shape[0] // 2, vector.shape[1]
    tall = rows * len(slots)
    me = lax.axis_index("pair").astype(jnp.int32)[None]

    def load(inputs, outs, scratch):
        outs[0][...] = inputs[0][0][...]

    (vector,) = kernel_call(load, [array(2 * rows, m)], [vector])
    table = tabulate(charges, coupling)
    *ops, edge = prepare(me, left_ops, right_ops, vector, count)
    column = double(vector, deep)
    divisor = double(divisor, deep)

    def part(inputs, outs, scratch):
        outs[0][...] = inputs[0][0][:tall, :]
        outs[1][...] = inputs[0][0][tall:, :]

    vector_a, vector_b = kernel_call(part, [array(tall, m)] * 2, [column])
    image = sigma_apply(vector_a, vector_b, ops, table, edge)
    for mask in deep[:0:-1]:

        def add_columns(inputs, outs, scratch):
            own, got = inputs[0]
            outs[0][...] = own[...] + turned(got[...], slots, mask, rows)

        (image,) = kernel_call(add_columns, [array(*image.shape)], [image, swap(image, mask)])

    def correct(inputs, outs, scratch):
        own, got, w_ref, p_ref = inputs[0]
        correction_a, correction_b, image_own, sums_out, edge_out = outs
        total = own[...] + turned(got[...], slots, deep[0], rows)
        sums = total[2 * tall :]
        theta = sums[0:1, :] / sums[1:2, :]
        c = (total[: 2 * tall] - theta * w_ref[...]) / p_ref[...]
        correction_a[...] = c[:tall]
        correction_b[...] = c[tall:]
        sums_out[...] = sums

        def owned(value):
            return jnp.concatenate([value[:rows], value[tall : tall + rows]], axis=0)

        own_w, own_c, own_a = owned(w_ref[...]), owned(c), owned(total)
        image_own[...] = own_a
        edge_out[...] = tile_rows(
            [jnp.zeros((1, m), F32), summed(own_w * own_c, m), summed(own_c * own_c, m), summed(own_a * own_c, m)]
        )

    ca, cb, image_own, sums, edge = kernel_call(
        correct, [array(tall, m), array(tall, m), array(2 * rows, m), array(EDGE, m), array(EDGE, m)],
        [image, swap(image, deep[0]), column, divisor],
    )
    own_c = (ca, cb)
    second = sigma_apply(ca, cb, ops, table, edge)

    for mask in deep[::-1]:
        size = (second.shape[0] - EDGE) // 4

        def cut(inputs, outs, scratch):
            ref, out = inputs[0][0], outs[0]
            out[:size, :] = ref[size : 2 * size, :]
            out[size:, :] = ref[3 * size :, :]

        def meet(inputs, outs, scratch):
            (ref, got), out = inputs[0], outs[0]
            out[:size, :] = ref[:size, :] + got[:size, :]
            out[size : 2 * size, :] = ref[2 * size : 3 * size, :] + got[size : 2 * size, :]
            out[2 * size :, :] = ref[4 * size :, :] + got[2 * size :, :]

        shape = [array(2 * size + EDGE, m)]
        (go,) = kernel_call(cut, shape, [second])
        (second,) = kernel_call(meet, shape, [second, swap(go, mask)])

    scale = math.sqrt(lax.axis_size("sector") * count * vector.shape[0] * m)

    def finish(inputs, outs, scratch):
        (second_ref,), (vector_ref, image_ref, ca_ref, cb_ref), (first_ref,) = inputs
        sums = second_ref[2 * rows :, :]
        correlation, norm_sq = first_ref[0:1, :], first_ref[1:2, :]
        theta = correlation / norm_sq
        inverse = lax.rsqrt(norm_sq)
        along = sums[1:2] / norm_sq
        length_sq = (sums[2:3] - along * sums[1:2]) / norm_sq
        factor = inverse * lax.rsqrt(length_sq + 1e-30)
        corner = factor * factor * (sums[0:1] - 2.0 * along * sums[3:4] + along * along * correlation)
        cross = inverse * factor * (sums[3:4] - along * correlation)
        spread = (theta - corner) / 2.0
        lowest = (theta + corner) / 2.0 - jnp.sqrt(spread * spread + cross * cross)
        first_weight = corner - lowest
        second_weight = -cross
        size_norm = jnp.sqrt(first_weight * first_weight + second_weight * second_weight + 1e-30)
        factor_two = scale * second_weight / size_norm * factor
        factor_one = scale * first_weight / size_norm * inverse - factor_two * along
        for at, c_ref in ((0, ca_ref), (rows, cb_ref)):
            span = slice(at, at + rows)
            outs[0][span, :] = factor_one * vector_ref[span, :] + factor_two * c_ref[:rows, :]
            outs[1][span, :] = factor_one * image_ref[span, :] + factor_two * second_ref[span, :]
        outs[2][0] = jnp.max(theta)
        outs[2][1] = jnp.max(lowest)

    state, image, energies = kernel_call(
        finish, [array(2 * rows, m), array(2 * rows, m), array(2)], [second],
        [vector, image_own, own_c[0], own_c[1]], [sums], scalar_outs=1,
    )
    return (state[None], image[None], energies)


def solution(mesh):
    in_specs = (
        P("sector", "pair", None),
        P("sector", "pair", None),
        P("pair", "sector", None, None),
        P("pair", "sector", None, None),
        P("pair"),
        P("sector", None),
    )
    out_specs = (P("sector", "pair", None), P("sector", "pair", None), P())
    return jax.shard_map(
        per_device, mesh=mesh, in_specs=in_specs, out_specs=out_specs, check_vma=False
    )
```

```python
import math

import jax
import jax.numpy as jnp
from jax import lax
from jax.experimental import pallas as pl
from jax.experimental.pallas import tpu as pltpu
from jax.sharding import PartitionSpec as P


F32, BF16 = jnp.float32, jnp.bfloat16
LIMIT = 12 * 1024 * 1024
PREPARE_LIMIT = 40 * 1024 * 1024
X, Y = 1, 2
EDGE = 8


def deep_masks(count):
    bits = [4 << b for b in range((count // 4).bit_length() - 1)]
    return bits[:1] + [bits[0] | bits[1]] + bits[2:] if len(bits) > 1 else bits


def streams(count):
    deep = deep_masks(count)
    return deep + [X, Y], deep + [Y, X]


def offsets(masks):
    slots = [0]
    for mask in masks:
        slots = slots + [slot ^ mask for slot in slots]
    return slots


def row_order(count):
    a, b = (offsets(masks) for masks in streams(count))
    middle = count // 2
    return (
        [(s, 0) for s in a[:middle]] + [(s, 1) for s in b[:middle]]
        + [(s, 0) for s in a[middle:]] + [(s, 1) for s in b[middle:]]
    )


def swap(block, mask):
    return lax.ppermute(block, "pair", [(i, i ^ mask) for i in range(lax.axis_size("pair"))])


def shifted(block, distance):
    size = lax.axis_size("sector")
    return lax.ppermute(block, "sector", [((i - distance) % size, i) for i in range(size)])


def neighbours(block):
    if lax.axis_size("sector") == 2:
        return [shifted(block, 1)]
    return [shifted(block, 1), shifted(block, -1)]


def to_neighbours(blocks):
    if lax.axis_size("sector") == 2:
        return [shifted(blocks[0], 1)]
    return [shifted(blocks[0], -1), shifted(blocks[1], 1)]


def over_sectors(tile):
    if lax.axis_size("sector") == 2:
        return [tile, shifted(tile, 1)]
    return [lax.psum(tile, "sector")]


def array(*shape, kind=F32):
    return jax.ShapeDtypeStruct(shape, kind)


def kernel_call(body, outs, *groups, scratch=(), flops=0, scalar_outs=0):
    flat = [value for group in groups for value in group]

    def kernel(*refs):
        refs = list(refs)
        take = lambda n: [refs.pop(0) for _ in range(n)]
        inputs = [take(len(group)) for group in groups]
        body(inputs, take(len(outs)), refs)

    traffic = sum(v.size * v.dtype.itemsize for v in flat)
    return pl.pallas_call(
        kernel,
        in_specs=[pl.BlockSpec(memory_space=pltpu.VMEM)] * len(flat),
        out_specs=[pl.BlockSpec(memory_space=pltpu.VMEM)] * (len(outs) - scalar_outs)
        + [pl.BlockSpec(memory_space=pltpu.SMEM)] * scalar_outs,
        out_shape=list(outs),
        scratch_shapes=list(scratch),
        compiler_params=pltpu.CompilerParams(vmem_limit_bytes=LIMIT),
        cost_estimate=pl.CostEstimate(flops=max(flops, traffic), bytes_accessed=traffic, transcendentals=0),
    )(*flat)


def split(value):
    high = value.astype(BF16)
    return high, (value - high.astype(F32)).astype(BF16)


def dot(first, second):
    return jnp.dot(first, second, preferred_element_type=F32)


def dot3(first, second):
    return dot(first[0], second[0]) + dot(first[0], second[1]) + dot(first[1], second[0])


def tile_rows(values):
    shape = (EDGE, values[0].shape[1])
    row = lax.broadcasted_iota(jnp.int32, shape, 0)
    tile = jnp.zeros(shape, F32)
    for at, value in enumerate(values):
        tile = jnp.where(row == at, value, tile)
    return tile


def summed(value, width):
    return jnp.broadcast_to(jnp.sum(value, keepdims=True), (1, width))


def block_of(charge, sectors):
    return jnp.where(charge == 1, 0, 1 if sectors == 2 else jnp.where(charge == 0, 1, 2))


def tabulate(charges, coupling):
    pairs, sectors = charges.shape[0], lax.axis_size("sector")

    def kernel(charges_ref, coupling_ref, table):
        row = lax.broadcasted_iota(jnp.int32, table.shape, 0)
        values = jnp.zeros(table.shape, jnp.int32)
        for pair in range(pairs):
            charge = charges_ref[pair]
            values = jnp.where(row == 2 * pair, block_of(charge, sectors), values)
            values = jnp.where(row == 2 * pair + 1, coupling_ref[0, charge], values)
        table[...] = values

    return pl.pallas_call(
        kernel,
        in_specs=[pl.BlockSpec(memory_space=pltpu.SMEM)] * 2,
        out_specs=pl.BlockSpec(memory_space=pltpu.VMEM),
        out_shape=array(-(-2 * pairs // 8) * 8, 128, kind=jnp.int32),
        compiler_params=pltpu.CompilerParams(vmem_limit_bytes=LIMIT),
        cost_estimate=pl.CostEstimate(flops=10**6, bytes_accessed=4096, transcendentals=0),
    )(charges, coupling)


def prepare(me, left_ops, right_ops, block, count):
    pairs, _, m, _ = left_ops.shape
    rows = m // count // 2
    order = row_order(count)

    def kernel(me_ref, left_ref, right_ref, block_ref, *refs):
        left_out, left_t_out, right_out, right_t_out, edge, held = refs

        def reorder(value):
            held[...] = value
            parts = []
            for slot, half in order:
                where = pl.multiple_of((me_ref[0] ^ slot) * (2 * rows) + half * rows, rows)
                parts.append(held[pl.ds(where, rows), :])
            return jnp.concatenate(parts, axis=0)

        turned = reorder(reorder(left_ref[...]).T)
        left_t_out[0], left_t_out[1] = split(turned)
        left_out[0], left_out[1] = split(turned.T)
        value = right_ref[...]
        right_out[0], right_out[1] = split(value)
        right_t_out[0], right_t_out[1] = split(value.T)
        edge[...] = tile_rows([jnp.zeros((1, m), F32), summed(block_ref[...] * block_ref[...], m)])

    source = pl.BlockSpec((None, None, m, m), lambda p, *_: (p, 0, 0, 0))
    target = pl.BlockSpec((None, 2, m, m), lambda p, *_: (p, 0, 0, 0))
    whole = pl.BlockSpec(memory_space=pltpu.VMEM)
    return pl.pallas_call(
        kernel,
        grid_spec=pltpu.PrefetchScalarGridSpec(
            num_scalar_prefetch=1,
            grid=(pairs,),
            in_specs=[source, source, whole],
            out_specs=[target] * 4 + [whole],
            scratch_shapes=[pltpu.VMEM((m, m), F32)],
        ),
        out_shape=[array(pairs, 2, m, m, kind=BF16)] * 4 + [array(EDGE, m)],
        compiler_params=pltpu.CompilerParams(vmem_limit_bytes=PREPARE_LIMIT),
        cost_estimate=pl.CostEstimate(flops=pairs * m * m * 1500, bytes_accessed=24 * pairs * m * m, transcendentals=0),
    )(me, left_ops, right_ops, block)


def double(block, masks):
    for mask in masks:
        more = swap(block, mask)
        rows, m = block.shape[0] // 2, block.shape[1]

        def meet_column(inputs, outs, scratch):
            (low, high), (out,) = inputs[0], outs
            for part in (0, 1):
                span = slice(part * rows, (part + 1) * rows)
                out[2 * part * rows : (2 * part + 1) * rows, :] = low[span, :]
                out[(2 * part + 1) * rows : (2 * part + 2) * rows, :] = high[span, :]

        (block,) = kernel_call(meet_column, [array(4 * rows, m)], [block, more])
    return block


def sigma_apply(column_a, column_b, ops, table, edge, halves):
    left, left_t, right, right_t = ops
    pairs, m = left.shape[0], left.shape[2]
    sectors = lax.axis_size("sector")
    blocks = min(sectors, 3)
    half, quarter, eighth = m // 2, m // 4, m // 8
    rows_of = array(half, m)
    made = array(pairs, 2, half, m, kind=BF16)
    held = pltpu.VMEM((blocks, 2, half, m), BF16)
    cost = 6 * half * m * m * pairs

    def hold(scratch, groups):
        for block, group in enumerate(groups):
            at = 0
            for ref in group:
                size = ref.shape[0]
                scratch[block, 0, at : at + size, :], scratch[block, 1, at : at + size, :] = split(ref[...])
                at += size

    def gains(fixed, pair):
        block = jnp.max(fixed[2 * pair : 2 * pair + 1, :])
        return block, fixed[2 * pair + 1 : 2 * pair + 2, :1].astype(F32)

    def parts(ref, *index):
        return ref[index[0], 0], ref[index[0], 1]

    more_a, more_b = swap(column_a, X), swap(column_b, Y)

    def join(inputs, outs, scratch):
        both, a, b = outs
        for at, (low, high), out in ((0, inputs[0], a), (quarter, inputs[1], b)):
            out[:eighth, :] = low[...]
            out[eighth:, :] = high[...]
            both[at : at + eighth, :] = low[...]
            both[at + eighth : at + quarter, :] = high[...]

    early, a, b = kernel_call(
        join, [rows_of, array(quarter, m), array(quarter, m)], [column_a, more_a], [column_b, more_b]
    )
    early_others = neighbours(early)
    late = [swap(a, Y), swap(b, X)]

    def outer(ref, pair, at, start, inner):
        rows, columns = slice(at, at + half), slice(start, start + half)
        return dot3((ref[pair, 0, rows, columns], ref[pair, 1, rows, columns]), inner)

    def first_inner(inputs, outs, scratch):
        (own, *others), (rights,), (rights_t,), (lefts,), (lefts_t,), (fixed,) = inputs
        z_out, y_out, back_out = outs[:3]
        held_ref, total = scratch
        hold(held_ref, [[own]] + [[other] for other in others])
        total[...] = jnp.zeros_like(total)
        back = jnp.zeros((half, m), F32)
        for pair in range(pairs):
            block, allowed = gains(fixed, pair)
            forward = split(dot3(parts(held_ref, 0), parts(rights_t, pair)) * allowed)
            z_out[pair, 0], z_out[pair, 1] = forward
            total[block] = total[block] + outer(lefts, pair, half, 0, forward)
            backward = split(dot3((held_ref[block, 0], held_ref[block, 1]), parts(rights, pair)) * allowed)
            y_out[pair, 0], y_out[pair, 1] = backward
            back = back + outer(lefts_t, pair, half, 0, backward)
        back_out[...] = back
        for block in range(blocks):
            outs[3 + block][...] = total[block]

    totals = pltpu.VMEM((blocks, half, m), F32)
    early_z, early_y, early_back, *early_terms = kernel_call(
        first_inner, [made] * 2 + [rows_of] * (1 + blocks), [early] + early_others, [right], [right_t], [left],
        [left_t], [table], scratch=[held, totals], flops=3 * cost,
    )
    late_others = [neighbours(piece) for piece in late]
    late_others = [[late_others[q][b] for q in range(2)] for b in range(blocks - 1)]

    def forward_late(inputs, outs, scratch):
        own, terms, (rights_t,), (lefts,), (fixed,) = inputs
        z_out, (held_ref, total) = outs[0], scratch
        hold(held_ref, [own])
        for block in range(blocks):
            total[block] = terms[block][...]
        for pair in range(pairs):
            block, allowed = gains(fixed, pair)
            inner = split(dot3(parts(held_ref, 0), parts(rights_t, pair)) * allowed)
            z_out[pair, 0], z_out[pair, 1] = inner
            total[block] = total[block] + outer(lefts, pair, half, half, inner)
        for block in range(blocks):
            outs[1 + block][...] = total[block]

    late_z, own_sent, *aimed = kernel_call(
        forward_late, [made] + [rows_of] * blocks, late, early_terms, [right_t], [left], [table],
        scratch=[held, totals], flops=2 * cost,
    )
    aimed_sent = to_neighbours(aimed)

    def backward_late(inputs, outs, scratch):
        groups, (rights,), (lefts_t,), (base, back_ref), (fixed,) = inputs
        y_out, sent, product = outs
        hold(scratch[0], [groups[2 * block : 2 * block + 2] for block in range(blocks)])
        total = back_ref[...]
        for pair in range(pairs):
            block, allowed = gains(fixed, pair)
            inner = split(dot3((scratch[0][block, 0], scratch[0][block, 1]), parts(rights, pair)) * allowed)
            y_out[pair, 0], y_out[pair, 1] = inner
            total = total + outer(lefts_t, pair, half, half, inner)
        sent[...] = total + base[...]
        own = jnp.concatenate([groups[0][...], groups[1][...]], axis=0)
        product[...] = jnp.broadcast_to(summed(own * total, m), (EDGE, m))

    late_y, own_sent, product = kernel_call(
        backward_late, [made, rows_of, array(EDGE, m)], late + sum(late_others, []), [right], [left_t],
        [own_sent, early_back], [table], scratch=[held], flops=2 * cost,
    )

    def add_sent(inputs, outs, scratch):
        value = sum(ref[...] for ref in inputs[0])
        outs[0][...] = value[:quarter]
        outs[1][...] = value[quarter:]

    sent_a, sent_b = kernel_call(add_sent, [array(quarter, m)] * 2, [own_sent] + aimed_sent)
    got_a, got_b = swap(sent_a, Y), swap(sent_b, X)

    def keep(inputs, outs, scratch):
        (z0, z1), (y0, y1), (lefts,), (lefts_t,), (own, product_ref, edge_ref), (fixed,) = inputs
        total = scratch[0]
        total[...] = jnp.zeros_like(total)
        back = jnp.zeros((half, m), F32)
        for pair in range(pairs):
            block, _ = gains(fixed, pair)
            term = outer(lefts, pair, 0, 0, parts(z0, pair)) + outer(lefts, pair, 0, half, parts(z1, pair))
            total[block] = total[block] + term
        for block in range(1, blocks):
            outs[1 + block][...] = total[block]
        for pair in range(pairs):
            back = back + outer(lefts_t, pair, 0, 0, parts(y0, pair))
            back = back + outer(lefts_t, pair, 0, half, parts(y1, pair))
        outs[0][...] = total[0] + back
        product_sum = 2.0 * (summed(own[...] * back, m) + product_ref[:1, :])
        row = lax.broadcasted_iota(jnp.int32, (EDGE, m), 0)
        outs[1][...] = jnp.where(row == 0, product_sum, edge_ref[...])

    own_kept, edge, *aimed = kernel_call(
        keep, [rows_of, array(EDGE, m)] + [rows_of] * (blocks - 1), [early_z, late_z], [early_y, late_y], [left],
        [left_t], [early, product, edge], [table],
        scratch=[totals], flops=2 * cost,
    )
    aimed_kept = to_neighbours(aimed)
    edges = over_sectors(edge)

    def first_sum(inputs, outs, scratch):
        kept, (a_ref, b_ref), edge_refs = inputs
        value = sum(ref[...] for ref in kept)
        edge_sum = sum(ref[...] for ref in edge_refs)
        a_value, b_value = value[:quarter] + a_ref[...], value[quarter:] + b_ref[...]
        for (stay, go), total in ((outs[:2], a_value), (outs[2:4], b_value)):
            stay[...] = total[:eighth]
            go[:eighth, :] = total[eighth:]
            go[eighth:, :] = edge_sum
        outs[4][...] = edge_sum

    stay_a, go_a, stay_b, go_b, edge = kernel_call(
        first_sum, [array(eighth, m), array(eighth + EDGE, m)] * 2 + [array(EDGE, m)],
        [own_kept] + aimed_kept, [got_a, got_b], edges,
    )
    got_a, got_b, corner = swap(go_a, X), swap(go_b, Y), swap(edge, X | Y)

    def second_sums(inputs, outs, scratch):
        (a_stay, a_got), (b_stay, b_got), (edge_ref, corner_ref) = inputs
        outs[0][:eighth, :] = a_stay[...] + a_got[:eighth, :]
        outs[0][eighth:, :] = edge_ref[...] + a_got[eighth:, :] + b_got[eighth:, :] + corner_ref[...]
        outs[1][...] = b_stay[...] + b_got[:eighth, :]

    if halves:
        shapes = [array(eighth + EDGE, m), array(eighth, m)]
        return kernel_call(second_sums, shapes, [stay_a, got_a], [stay_b, got_b], [edge, corner])

    def second_sum(inputs, outs, scratch):
        (a_stay, a_got), (b_stay, b_got), (edge_ref, corner_ref) = inputs
        outs[0][:eighth, :] = a_stay[...] + a_got[:eighth, :]
        outs[0][eighth:quarter, :] = b_stay[...] + b_got[:eighth, :]
        outs[0][quarter:, :] = edge_ref[...] + a_got[eighth:, :] + b_got[eighth:, :] + corner_ref[...]

    return kernel_call(second_sum, [array(quarter + EDGE, m)], [stay_a, got_a], [stay_b, got_b], [edge, corner])[0]


def turned(value, slots, mask, rows):
    size = len(slots) * rows
    parts = [value[slots.index(slot ^ mask) * rows :][:rows] for slot in slots]
    return jnp.concatenate(parts + ([value[size:]] if value.shape[0] > size else []), axis=0)


def per_device(wavefunction, preconditioner, left_ops, right_ops, charges, coupling):
    vector, divisor = wavefunction[0], preconditioner[0]
    count = lax.axis_size("pair")
    deep = deep_masks(count)
    slots = offsets(deep)
    rows, m = vector.shape[0] // 2, vector.shape[1]
    tall = rows * len(slots)
    me = lax.axis_index("pair").astype(jnp.int32)[None]

    def load(inputs, outs, scratch):
        outs[0][...] = inputs[0][0][...]

    (vector,) = kernel_call(load, [array(2 * rows, m)], [vector])
    table = tabulate(charges, coupling)
    *ops, edge = prepare(me, left_ops, right_ops, vector, count)
    column = double(vector, deep)
    divisor = double(divisor, deep)

    def part(inputs, outs, scratch):
        outs[0][...] = inputs[0][0][:tall, :]
        outs[1][...] = inputs[0][0][tall:, :]

    vector_a, vector_b = kernel_call(part, [array(tall, m)] * 2, [column])
    image_a, image_b = sigma_apply(vector_a, vector_b, ops, table, edge, True)
    for masks in zip(deep[:0:-1], deep[:-1]):

        def add_columns(inputs, outs, scratch):
            for (own, got), out, mask in zip(inputs, outs, masks):
                out[...] = own[...] + turned(got[...], slots, mask, rows)

        image_a, image_b = kernel_call(
            add_columns, [array(*image_a.shape), array(*image_b.shape)],
            [image_a, swap(image_a, masks[0])], [image_b, swap(image_b, masks[1])],
        )

    def correct(inputs, outs, scratch):
        a_ref, a_got, b_ref, b_got, w_ref, p_ref = inputs[0]
        correction_a, correction_b, image_own, sums_out, edge_out = outs
        total_a = a_ref[...] + turned(a_got[...], slots, deep[0], rows)
        total_b = b_ref[...] + turned(b_got[...], slots, deep[-1], rows)
        total = jnp.concatenate([total_a[:tall], total_b, total_a[tall:]], axis=0)
        sums = total[2 * tall :]
        theta = sums[0:1, :] / sums[1:2, :]
        c = (total[: 2 * tall] - theta * w_ref[...]) / p_ref[...]
        correction_a[...] = c[:tall]
        correction_b[...] = c[tall:]
        sums_out[...] = sums

        def owned(value):
            return jnp.concatenate([value[:rows], value[tall : tall + rows]], axis=0)

        own_w, own_c, own_a = owned(w_ref[...]), owned(c), owned(total)
        image_own[...] = own_a
        edge_out[...] = tile_rows(
            [jnp.zeros((1, m), F32), summed(own_w * own_c, m), summed(own_c * own_c, m), summed(own_a * own_c, m)]
        )

    ca, cb, image_own, sums, edge = kernel_call(
        correct, [array(tall, m), array(tall, m), array(2 * rows, m), array(EDGE, m), array(EDGE, m)],
        [image_a, swap(image_a, deep[0]), image_b, swap(image_b, deep[-1]), column, divisor],
    )
    own_c = (ca, cb)
    second = sigma_apply(ca, cb, ops, table, edge, False)

    for mask in deep[::-1]:
        size = (second.shape[0] - EDGE) // 4

        def cut(inputs, outs, scratch):
            ref, out = inputs[0][0], outs[0]
            out[:size, :] = ref[size : 2 * size, :]
            out[size:, :] = ref[3 * size :, :]

        def meet(inputs, outs, scratch):
            (ref, got), out = inputs[0], outs[0]
            out[:size, :] = ref[:size, :] + got[:size, :]
            out[size : 2 * size, :] = ref[2 * size : 3 * size, :] + got[size : 2 * size, :]
            out[2 * size :, :] = ref[4 * size :, :] + got[2 * size :, :]

        shape = [array(2 * size + EDGE, m)]
        (go,) = kernel_call(cut, shape, [second])
        (second,) = kernel_call(meet, shape, [second, swap(go, mask)])

    scale = math.sqrt(lax.axis_size("sector") * count * vector.shape[0] * m)

    def finish(inputs, outs, scratch):
        (second_ref,), (vector_ref, image_ref, ca_ref, cb_ref), (first_ref,) = inputs
        sums = second_ref[2 * rows :, :]
        correlation, norm_sq = first_ref[0:1, :], first_ref[1:2, :]
        theta = correlation / norm_sq
        inverse = lax.rsqrt(norm_sq)
        along = sums[1:2] / norm_sq
        length_sq = (sums[2:3] - along * sums[1:2]) / norm_sq
        factor = inverse * lax.rsqrt(length_sq + 1e-30)
        corner = factor * factor * (sums[0:1] - 2.0 * along * sums[3:4] + along * along * correlation)
        cross = inverse * factor * (sums[3:4] - along * correlation)
        spread = (theta - corner) / 2.0
        lowest = (theta + corner) / 2.0 - jnp.sqrt(spread * spread + cross * cross)
        first_weight = corner - lowest
        second_weight = -cross
        size_norm = jnp.sqrt(first_weight * first_weight + second_weight * second_weight + 1e-30)
        factor_two = scale * second_weight / size_norm * factor
        factor_one = scale * first_weight / size_norm * inverse - factor_two * along
        for at, c_ref in ((0, ca_ref), (rows, cb_ref)):
            span = slice(at, at + rows)
            outs[0][span, :] = factor_one * vector_ref[span, :] + factor_two * c_ref[:rows, :]
            outs[1][span, :] = factor_one * image_ref[span, :] + factor_two * second_ref[span, :]
        outs[2][0] = jnp.max(theta)
        outs[2][1] = jnp.max(lowest)

    state, image, energies = kernel_call(
        finish, [array(2 * rows, m), array(2 * rows, m), array(2)], [second],
        [vector, image_own, own_c[0], own_c[1]], [sums], scalar_outs=1,
    )
    return (state[None], image[None], energies)


def solution(mesh):
    in_specs = (
        P("sector", "pair", None),
        P("sector", "pair", None),
        P("pair", "sector", None, None),
        P("pair", "sector", None, None),
        P("pair"),
        P("sector", None),
    )
    out_specs = (P("sector", "pair", None), P("sector", "pair", None), P())
    return jax.shard_map(
        per_device, mesh=mesh, in_specs=in_specs, out_specs=out_specs, check_vma=False
    )
```

```python
import math

import jax
import jax.numpy as jnp
from jax import lax
from jax.experimental import pallas as pl
from jax.experimental.pallas import tpu as pltpu
from jax.sharding import PartitionSpec as P


F32, BF16 = jnp.float32, jnp.bfloat16
LIMIT = 12 * 1024 * 1024
PREPARE_LIMIT = 40 * 1024 * 1024
X, Y = 1, 2
EDGE = 8


def deep_masks(count):
    bits = [4 << b for b in range((count // 4).bit_length() - 1)]
    return bits[:1] + [bits[0] | bits[1]] + bits[2:] if len(bits) > 1 else bits


def streams(count):
    deep = deep_masks(count)
    return deep + [X, Y], deep + [Y, X]


def offsets(masks):
    slots = [0]
    for mask in masks:
        slots = slots + [slot ^ mask for slot in slots]
    return slots


def row_order(count):
    a, b = (offsets(masks) for masks in streams(count))
    middle = count // 2
    return (
        [(s, 0) for s in a[:middle]] + [(s, 1) for s in b[:middle]]
        + [(s, 0) for s in a[middle:]] + [(s, 1) for s in b[middle:]]
    )


def swap(block, mask):
    return lax.ppermute(block, "pair", [(i, i ^ mask) for i in range(lax.axis_size("pair"))])


def shifted(block, distance):
    size = lax.axis_size("sector")
    return lax.ppermute(block, "sector", [((i - distance) % size, i) for i in range(size)])


def neighbours(block):
    if lax.axis_size("sector") == 2:
        return [shifted(block, 1)]
    return [shifted(block, 1), shifted(block, -1)]


def to_neighbours(blocks):
    if lax.axis_size("sector") == 2:
        return [shifted(blocks[0], 1)]
    return [shifted(blocks[0], -1), shifted(blocks[1], 1)]


def over_sectors(tile):
    if lax.axis_size("sector") == 2:
        return [tile, shifted(tile, 1)]
    return [lax.psum(tile, "sector")]


def array(*shape, kind=F32):
    return jax.ShapeDtypeStruct(shape, kind)


def kernel_call(body, outs, *groups, scratch=(), flops=0, scalar_outs=0):
    flat = [value for group in groups for value in group]

    def kernel(*refs):
        refs = list(refs)
        take = lambda n: [refs.pop(0) for _ in range(n)]
        inputs = [take(len(group)) for group in groups]
        body(inputs, take(len(outs)), refs)

    traffic = sum(v.size * v.dtype.itemsize for v in flat)
    return pl.pallas_call(
        kernel,
        in_specs=[pl.BlockSpec(memory_space=pltpu.VMEM)] * len(flat),
        out_specs=[pl.BlockSpec(memory_space=pltpu.VMEM)] * (len(outs) - scalar_outs)
        + [pl.BlockSpec(memory_space=pltpu.SMEM)] * scalar_outs,
        out_shape=list(outs),
        scratch_shapes=list(scratch),
        compiler_params=pltpu.CompilerParams(vmem_limit_bytes=LIMIT),
        cost_estimate=pl.CostEstimate(flops=max(flops, traffic), bytes_accessed=traffic, transcendentals=0),
    )(*flat)


def split(value):
    high = value.astype(BF16)
    return high, (value - high.astype(F32)).astype(BF16)


def dot(first, second):
    return jnp.dot(first, second, preferred_element_type=F32)


def dot3(first, second):
    return dot(first[0], second[0]) + dot(first[0], second[1]) + dot(first[1], second[0])


def tile_rows(values):
    shape = (EDGE, values[0].shape[1])
    row = lax.broadcasted_iota(jnp.int32, shape, 0)
    tile = jnp.zeros(shape, F32)
    for at, value in enumerate(values):
        tile = jnp.where(row == at, value, tile)
    return tile


def summed(value, width):
    return jnp.broadcast_to(jnp.sum(value, keepdims=True), (1, width))


def block_of(charge, sectors):
    return jnp.where(charge == 1, 0, 1 if sectors == 2 else jnp.where(charge == 0, 1, 2))


def tabulate(charges, coupling):
    pairs, sectors = charges.shape[0], lax.axis_size("sector")

    def kernel(charges_ref, coupling_ref, table):
        row = lax.broadcasted_iota(jnp.int32, table.shape, 0)
        values = jnp.zeros(table.shape, jnp.int32)
        for pair in range(pairs):
            charge = charges_ref[pair]
            values = jnp.where(row == 2 * pair, block_of(charge, sectors), values)
            values = jnp.where(row == 2 * pair + 1, coupling_ref[0, charge], values)
        table[...] = values

    return pl.pallas_call(
        kernel,
        in_specs=[pl.BlockSpec(memory_space=pltpu.SMEM)] * 2,
        out_specs=pl.BlockSpec(memory_space=pltpu.VMEM),
        out_shape=array(-(-2 * pairs // 8) * 8, 128, kind=jnp.int32),
        compiler_params=pltpu.CompilerParams(vmem_limit_bytes=LIMIT),
        cost_estimate=pl.CostEstimate(flops=10**6, bytes_accessed=4096, transcendentals=0),
    )(charges, coupling)


def prepare(me, left_ops, right_ops, block, count):
    pairs, _, m, _ = left_ops.shape
    rows = m // count // 2
    order = row_order(count)

    def kernel(me_ref, left_ref, right_ref, block_ref, *refs):
        left_out, left_t_out, right_out, right_t_out, edge, held = refs

        def reorder(value):
            held[...] = value
            parts = []
            for slot, half in order:
                where = pl.multiple_of((me_ref[0] ^ slot) * (2 * rows) + half * rows, rows)
                parts.append(held[pl.ds(where, rows), :])
            return jnp.concatenate(parts, axis=0)

        turned = reorder(reorder(left_ref[...]).T)
        left_t_out[0], left_t_out[1] = split(turned)
        left_out[0], left_out[1] = split(turned.T)
        value = right_ref[...]
        right_out[0], right_out[1] = split(value)
        right_t_out[0], right_t_out[1] = split(value.T)
        edge[...] = tile_rows([jnp.zeros((1, m), F32), summed(block_ref[...] * block_ref[...], m)])

    source = pl.BlockSpec((None, None, m, m), lambda p, *_: (p, 0, 0, 0))
    target = pl.BlockSpec((None, 2, m, m), lambda p, *_: (p, 0, 0, 0))
    whole = pl.BlockSpec(memory_space=pltpu.VMEM)
    return pl.pallas_call(
        kernel,
        grid_spec=pltpu.PrefetchScalarGridSpec(
            num_scalar_prefetch=1,
            grid=(pairs,),
            in_specs=[source, source, whole],
            out_specs=[target] * 4 + [whole],
            scratch_shapes=[pltpu.VMEM((m, m), F32)],
        ),
        out_shape=[array(pairs, 2, m, m, kind=BF16)] * 4 + [array(EDGE, m)],
        compiler_params=pltpu.CompilerParams(vmem_limit_bytes=PREPARE_LIMIT),
        cost_estimate=pl.CostEstimate(flops=pairs * m * m * 1500, bytes_accessed=24 * pairs * m * m, transcendentals=0),
    )(me, left_ops, right_ops, block)


def double(block, masks, first=None):
    for step, mask in enumerate(masks):
        more = swap(first if step == 0 and first is not None else block, mask)
        rows, m = block.shape[0] // 2, block.shape[1]

        def meet_column(inputs, outs, scratch):
            (low, high), (out,) = inputs[0], outs
            for part in (0, 1):
                span = slice(part * rows, (part + 1) * rows)
                out[2 * part * rows : (2 * part + 1) * rows, :] = low[span, :]
                out[(2 * part + 1) * rows : (2 * part + 2) * rows, :] = high[span, :]

        (block,) = kernel_call(meet_column, [array(4 * rows, m)], [block, more])
    return block


def sigma_apply(column_a, column_b, ops, table, edge, halves):
    left, left_t, right, right_t = ops
    pairs, m = left.shape[0], left.shape[2]
    sectors = lax.axis_size("sector")
    blocks = min(sectors, 3)
    half, quarter, eighth = m // 2, m // 4, m // 8
    rows_of = array(half, m)
    made = array(pairs, 2, half, m, kind=BF16)
    held = pltpu.VMEM((blocks, 2, half, m), BF16)
    cost = 6 * half * m * m * pairs

    def hold(scratch, groups):
        for block, group in enumerate(groups):
            at = 0
            for ref in group:
                size = ref.shape[0]
                scratch[block, 0, at : at + size, :], scratch[block, 1, at : at + size, :] = split(ref[...])
                at += size

    def gains(fixed, pair):
        block = jnp.max(fixed[2 * pair : 2 * pair + 1, :])
        return block, fixed[2 * pair + 1 : 2 * pair + 2, :1].astype(F32)

    def parts(ref, *index):
        return ref[index[0], 0], ref[index[0], 1]

    more_a, more_b = swap(column_a, X), swap(column_b, Y)

    def join(inputs, outs, scratch):
        both, a, b = outs
        for at, (low, high), out in ((0, inputs[0], a), (quarter, inputs[1], b)):
            out[:eighth, :] = low[...]
            out[eighth:, :] = high[...]
            both[at : at + eighth, :] = low[...]
            both[at + eighth : at + quarter, :] = high[...]

    early, a, b = kernel_call(
        join, [rows_of, array(quarter, m), array(quarter, m)], [column_a, more_a], [column_b, more_b]
    )
    early_others = neighbours(early)
    late = [swap(a, Y), swap(b, X)]

    def outer(ref, pair, at, start, inner):
        rows, columns = slice(at, at + half), slice(start, start + half)
        return dot3((ref[pair, 0, rows, columns], ref[pair, 1, rows, columns]), inner)

    def first_inner(inputs, outs, scratch):
        (own, *others), (rights,), (rights_t,), (lefts,), (lefts_t,), (fixed,) = inputs
        z_out, y_out, back_out = outs[:3]
        held_ref, total = scratch
        hold(held_ref, [[own]] + [[other] for other in others])
        total[...] = jnp.zeros_like(total)
        back = jnp.zeros((half, m), F32)
        for pair in range(pairs):
            block, allowed = gains(fixed, pair)
            forward = split(dot3(parts(held_ref, 0), parts(rights_t, pair)) * allowed)
            z_out[pair, 0], z_out[pair, 1] = forward
            total[block] = total[block] + outer(lefts, pair, half, 0, forward)
            backward = split(dot3((held_ref[block, 0], held_ref[block, 1]), parts(rights, pair)) * allowed)
            y_out[pair, 0], y_out[pair, 1] = backward
            back = back + outer(lefts_t, pair, half, 0, backward)
        back_out[...] = back
        for block in range(blocks):
            outs[3 + block][...] = total[block]

    totals = pltpu.VMEM((blocks, half, m), F32)
    early_z, early_y, early_back, *early_terms = kernel_call(
        first_inner, [made] * 2 + [rows_of] * (1 + blocks), [early] + early_others, [right], [right_t], [left],
        [left_t], [table], scratch=[held, totals], flops=3 * cost,
    )
    late_others = [neighbours(piece) for piece in late]
    late_others = [[late_others[q][b] for q in range(2)] for b in range(blocks - 1)]

    def forward_late(inputs, outs, scratch):
        own, terms, (rights_t,), (lefts,), (fixed,) = inputs
        z_out, (held_ref, total) = outs[0], scratch
        hold(held_ref, [own])
        for block in range(blocks):
            total[block] = terms[block][...]
        for pair in range(pairs):
            block, allowed = gains(fixed, pair)
            inner = split(dot3(parts(held_ref, 0), parts(rights_t, pair)) * allowed)
            z_out[pair, 0], z_out[pair, 1] = inner
            total[block] = total[block] + outer(lefts, pair, half, half, inner)
        for block in range(blocks):
            outs[1 + block][...] = total[block]

    late_z, own_sent, *aimed = kernel_call(
        forward_late, [made] + [rows_of] * blocks, late, early_terms, [right_t], [left], [table],
        scratch=[held, totals], flops=2 * cost,
    )
    aimed_sent = to_neighbours(aimed)

    def backward_late(inputs, outs, scratch):
        groups, (rights,), (lefts_t,), (base, back_ref), (fixed,) = inputs
        y_out, sent, product = outs
        hold(scratch[0], [groups[2 * block : 2 * block + 2] for block in range(blocks)])
        total = back_ref[...]
        for pair in range(pairs):
            block, allowed = gains(fixed, pair)
            inner = split(dot3((scratch[0][block, 0], scratch[0][block, 1]), parts(rights, pair)) * allowed)
            y_out[pair, 0], y_out[pair, 1] = inner
            total = total + outer(lefts_t, pair, half, half, inner)
        sent[...] = total + base[...]
        own = jnp.concatenate([groups[0][...], groups[1][...]], axis=0)
        product[...] = jnp.broadcast_to(summed(own * total, m), (EDGE, m))

    late_y, own_sent, product = kernel_call(
        backward_late, [made, rows_of, array(EDGE, m)], late + sum(late_others, []), [right], [left_t],
        [own_sent, early_back], [table], scratch=[held], flops=2 * cost,
    )

    def add_sent(inputs, outs, scratch):
        value = sum(ref[...] for ref in inputs[0])
        outs[0][...] = value[:quarter]
        outs[1][...] = value[quarter:]

    sent_a, sent_b = kernel_call(add_sent, [array(quarter, m)] * 2, [own_sent] + aimed_sent)
    got_a, got_b = swap(sent_a, Y), swap(sent_b, X)

    def keep(inputs, outs, scratch):
        (z0, z1), (y0, y1), (lefts,), (lefts_t,), (own, product_ref, edge_ref), (fixed,) = inputs
        total = scratch[0]
        total[...] = jnp.zeros_like(total)
        back = jnp.zeros((half, m), F32)
        for pair in range(pairs):
            block, _ = gains(fixed, pair)
            term = outer(lefts, pair, 0, 0, parts(z0, pair)) + outer(lefts, pair, 0, half, parts(z1, pair))
            total[block] = total[block] + term
        for block in range(1, blocks):
            outs[1 + block][...] = total[block]
        for pair in range(pairs):
            back = back + outer(lefts_t, pair, 0, 0, parts(y0, pair))
            back = back + outer(lefts_t, pair, 0, half, parts(y1, pair))
        outs[0][...] = total[0] + back
        product_sum = 2.0 * (summed(own[...] * back, m) + product_ref[:1, :])
        row = lax.broadcasted_iota(jnp.int32, (EDGE, m), 0)
        outs[1][...] = jnp.where(row == 0, product_sum, edge_ref[...])

    own_kept, edge, *aimed = kernel_call(
        keep, [rows_of, array(EDGE, m)] + [rows_of] * (blocks - 1), [early_z, late_z], [early_y, late_y], [left],
        [left_t], [early, product, edge], [table],
        scratch=[totals], flops=2 * cost,
    )
    aimed_kept = to_neighbours(aimed)
    edges = over_sectors(edge)

    def first_sum(inputs, outs, scratch):
        kept, (a_ref, b_ref), edge_refs = inputs
        value = sum(ref[...] for ref in kept)
        edge_sum = sum(ref[...] for ref in edge_refs)
        a_value, b_value = value[:quarter] + a_ref[...], value[quarter:] + b_ref[...]
        for (stay, go), total in ((outs[:2], a_value), (outs[2:4], b_value)):
            stay[...] = total[:eighth]
            go[:eighth, :] = total[eighth:]
            go[eighth:, :] = edge_sum
        outs[4][...] = edge_sum

    stay_a, go_a, stay_b, go_b, edge = kernel_call(
        first_sum, [array(eighth, m), array(eighth + EDGE, m)] * 2 + [array(EDGE, m)],
        [own_kept] + aimed_kept, [got_a, got_b], edges,
    )
    got_a, got_b, corner = swap(go_a, X), swap(go_b, Y), swap(edge, X | Y)

    def second_sums(inputs, outs, scratch):
        (a_stay, a_got), (b_stay, b_got), (edge_ref, corner_ref) = inputs
        outs[0][:eighth, :] = a_stay[...] + a_got[:eighth, :]
        outs[0][eighth:, :] = edge_ref[...] + a_got[eighth:, :] + b_got[eighth:, :] + corner_ref[...]
        outs[1][...] = b_stay[...] + b_got[:eighth, :]

    if halves:
        shapes = [array(eighth + EDGE, m), array(eighth, m)]
        return kernel_call(second_sums, shapes, [stay_a, got_a], [stay_b, got_b], [edge, corner])

    def second_sum(inputs, outs, scratch):
        (a_stay, a_got), (b_stay, b_got), (edge_ref, corner_ref) = inputs
        outs[0][:eighth, :] = a_stay[...] + a_got[:eighth, :]
        outs[0][eighth:quarter, :] = b_stay[...] + b_got[:eighth, :]
        outs[0][quarter:, :] = edge_ref[...] + a_got[eighth:, :] + b_got[eighth:, :] + corner_ref[...]

    return kernel_call(second_sum, [array(quarter + EDGE, m)], [stay_a, got_a], [stay_b, got_b], [edge, corner])[0]


def turned(value, slots, mask, rows):
    size = len(slots) * rows
    parts = [value[slots.index(slot ^ mask) * rows :][:rows] for slot in slots]
    return jnp.concatenate(parts + ([value[size:]] if value.shape[0] > size else []), axis=0)


def per_device(wavefunction, preconditioner, left_ops, right_ops, charges, coupling):
    vector, divisor = wavefunction[0], preconditioner[0]
    count = lax.axis_size("pair")
    deep = deep_masks(count)
    slots = offsets(deep)
    rows, m = vector.shape[0] // 2, vector.shape[1]
    tall = rows * len(slots)
    me = lax.axis_index("pair").astype(jnp.int32)[None]

    def load(inputs, outs, scratch):
        outs[0][...] = inputs[0][0][...]

    source = vector
    (vector,) = kernel_call(load, [array(2 * rows, m)], [vector])
    table = tabulate(charges, coupling)
    *ops, edge = prepare(me, left_ops, right_ops, vector, count)
    column = double(vector, deep, source)
    divisor = double(divisor, deep)

    def part(inputs, outs, scratch):
        outs[0][...] = inputs[0][0][:tall, :]
        outs[1][...] = inputs[0][0][tall:, :]

    vector_a, vector_b = kernel_call(part, [array(tall, m)] * 2, [column])
    image_a, image_b = sigma_apply(vector_a, vector_b, ops, table, edge, True)
    for masks in zip(deep[:0:-1], deep[:-1]):

        def add_columns(inputs, outs, scratch):
            for (own, got), out, mask in zip(inputs, outs, masks):
                out[...] = own[...] + turned(got[...], slots, mask, rows)

        image_a, image_b = kernel_call(
            add_columns, [array(*image_a.shape), array(*image_b.shape)],
            [image_a, swap(image_a, masks[0])], [image_b, swap(image_b, masks[1])],
        )

    def correct(inputs, outs, scratch):
        a_ref, a_got, b_ref, b_got, w_ref, p_ref = inputs[0]
        correction_a, correction_b, image_own, sums_out, edge_out = outs
        total_a = a_ref[...] + turned(a_got[...], slots, deep[0], rows)
        total_b = b_ref[...] + turned(b_got[...], slots, deep[-1], rows)
        total = jnp.concatenate([total_a[:tall], total_b, total_a[tall:]], axis=0)
        sums = total[2 * tall :]
        theta = sums[0:1, :] / sums[1:2, :]
        c = (total[: 2 * tall] - theta * w_ref[...]) / p_ref[...]
        correction_a[...] = c[:tall]
        correction_b[...] = c[tall:]
        sums_out[...] = sums

        def owned(value):
            return jnp.concatenate([value[:rows], value[tall : tall + rows]], axis=0)

        own_w, own_c, own_a = owned(w_ref[...]), owned(c), owned(total)
        image_own[...] = own_a
        edge_out[...] = tile_rows(
            [jnp.zeros((1, m), F32), summed(own_w * own_c, m), summed(own_c * own_c, m), summed(own_a * own_c, m)]
        )

    ca, cb, image_own, sums, edge = kernel_call(
        correct, [array(tall, m), array(tall, m), array(2 * rows, m), array(EDGE, m), array(EDGE, m)],
        [image_a, swap(image_a, deep[0]), image_b, swap(image_b, deep[-1]), column, divisor],
    )
    own_c = (ca, cb)
    second = sigma_apply(ca, cb, ops, table, edge, False)

    for mask in deep[::-1]:
        size = (second.shape[0] - EDGE) // 4

        def cut(inputs, outs, scratch):
            ref, out = inputs[0][0], outs[0]
            out[:size, :] = ref[size : 2 * size, :]
            out[size:, :] = ref[3 * size :, :]

        def meet(inputs, outs, scratch):
            (ref, got), out = inputs[0], outs[0]
            out[:size, :] = ref[:size, :] + got[:size, :]
            out[size : 2 * size, :] = ref[2 * size : 3 * size, :] + got[size : 2 * size, :]
            out[2 * size :, :] = ref[4 * size :, :] + got[2 * size :, :]

        shape = [array(2 * size + EDGE, m)]
        (go,) = kernel_call(cut, shape, [second])
        (second,) = kernel_call(meet, shape, [second, swap(go, mask)])

    scale = math.sqrt(lax.axis_size("sector") * count * vector.shape[0] * m)

    def finish(inputs, outs, scratch):
        (second_ref,), (vector_ref, image_ref, ca_ref, cb_ref), (first_ref,) = inputs
        sums = second_ref[2 * rows :, :]
        correlation, norm_sq = first_ref[0:1, :], first_ref[1:2, :]
        theta = correlation / norm_sq
        inverse = lax.rsqrt(norm_sq)
        along = sums[1:2] / norm_sq
        length_sq = (sums[2:3] - along * sums[1:2]) / norm_sq
        factor = inverse * lax.rsqrt(length_sq + 1e-30)
        corner = factor * factor * (sums[0:1] - 2.0 * along * sums[3:4] + along * along * correlation)
        cross = inverse * factor * (sums[3:4] - along * correlation)
        spread = (theta - corner) / 2.0
        lowest = (theta + corner) / 2.0 - jnp.sqrt(spread * spread + cross * cross)
        first_weight = corner - lowest
        second_weight = -cross
        size_norm = jnp.sqrt(first_weight * first_weight + second_weight * second_weight + 1e-30)
        factor_two = scale * second_weight / size_norm * factor
        factor_one = scale * first_weight / size_norm * inverse - factor_two * along
        for at, c_ref in ((0, ca_ref), (rows, cb_ref)):
            span = slice(at, at + rows)
            outs[0][span, :] = factor_one * vector_ref[span, :] + factor_two * c_ref[:rows, :]
            outs[1][span, :] = factor_one * image_ref[span, :] + factor_two * second_ref[span, :]
        outs[2][0] = jnp.max(theta)
        outs[2][1] = jnp.max(lowest)

    state, image, energies = kernel_call(
        finish, [array(2 * rows, m), array(2 * rows, m), array(2)], [second],
        [vector, image_own, own_c[0], own_c[1]], [sums], scalar_outs=1,
    )
    return (state[None], image[None], energies)


def solution(mesh):
    in_specs = (
        P("sector", "pair", None),
        P("sector", "pair", None),
        P("pair", "sector", None, None),
        P("pair", "sector", None, None),
        P("pair"),
        P("sector", None),
    )
    out_specs = (P("sector", "pair", None), P("sector", "pair", None), P())
    return jax.shard_map(
        per_device, mesh=mesh, in_specs=in_specs, out_specs=out_specs, check_vma=False
    )
```
